32 devices in a mesh: dp: 1 (over z), tp: 4 (over y), sp: 8 (over x, core).
Axes of the slice: x: 4, y: 4, z: 1, core: 2. Of those that a mesh axis runs over, the one named last changes fastest.
The devices are a block of a 4x4x8 slice.
Arguments:
- x_tokens: bfloat16 [2048, 8192], P(('dp', 'sp'), 'tp')
- doc_ids: int32 [2048], P(('dp', 'sp'))
- w_qkv: bfloat16 [8192, 24576], P('sp', 'tp')
- w_out: bfloat16 [8192, 8192], P('sp', 'tp')
Outputs:
- output: bfloat16 [2048, 8192], P(('dp', 'sp', 'tp'))
All inputs are finite; a program needn't handle non-finite values.
Results may differ from the reference program's by a relative error of at most 0.00311.
Values are sent between devices in bfloat16 or wider.
A program may use at most 768 MiB of HBM per device.

```python
import jax
import jax.numpy as jnp
from jax import lax

SEQ_LEN = 2048
HIDDEN = 8192
NUM_HEADS = 64
HEAD_DIM = 128
QUERY_BLOCK = 512
NUM_PIECES = 32
NUM_CUTS = 3

NUM_QBLOCKS = SEQ_LEN // QUERY_BLOCK
PIECE_LEN = SEQ_LEN // NUM_PIECES
SOFTMAX_SCALE = HEAD_DIM ** -0.5


def draw_segments(seg_key):
    cut_points = jax.random.randint(seg_key, (NUM_CUTS,), 1, SEQ_LEN)
    positions = jnp.arange(SEQ_LEN, dtype=jnp.int32)
    return jnp.sum((positions[:, None] >= cut_points[None, :]).astype(jnp.int32), axis=1).astype(jnp.int32)


def setup_inputs(seed: int = 0, part: int = 0) -> dict:
    base_key = jax.random.key(seed)
    part_key = jax.random.fold_in(base_key, part)
    noise_key, piece_key, seg_key = jax.random.split(part_key, 3)
    wqkv_key, wout_key = jax.random.split(jax.random.key(seed + 1), 2)
    x_noise = jax.random.normal(noise_key, (NUM_PIECES, PIECE_LEN, HIDDEN), jnp.float32)
    pieces = jax.random.normal(piece_key, (NUM_PIECES, 1, HIDDEN), jnp.float32)
    x_val = 0.6 * x_noise + 0.8 * pieces
    x_tokens = x_val.reshape(SEQ_LEN, HIDDEN).astype(jnp.bfloat16)
    w_qkv = (jax.random.normal(wqkv_key, (HIDDEN, 3 * HIDDEN), jnp.float32) * HIDDEN ** -0.5).astype(jnp.bfloat16)
    w_out = (jax.random.normal(wout_key, (HIDDEN, HIDDEN), jnp.float32) * (2.0 * HIDDEN ** -0.5)).astype(jnp.bfloat16)
    return {"x_tokens": x_tokens, "doc_ids": draw_segments(seg_key), "w_qkv": w_qkv, "w_out": w_out}


def reference(x_tokens, doc_ids, w_qkv, w_out):
    qkv_all = jnp.dot(x_tokens, w_qkv, preferred_element_type=jnp.float32).astype(jnp.bfloat16)
    per_head = qkv_all.reshape(SEQ_LEN, NUM_HEADS, 3, HEAD_DIM).transpose(1, 2, 0, 3).astype(jnp.float32)
    doc_blocks = doc_ids.reshape(NUM_QBLOCKS, QUERY_BLOCK)

    def head_attention(head_qkv):
        key_head = head_qkv[1]
        value_head = head_qkv[2]
        query_blocks = head_qkv[0].reshape(NUM_QBLOCKS, QUERY_BLOCK, HEAD_DIM)

        def block_attention(block):
            query_blk, doc_blk = block
            scores = jnp.dot(query_blk, key_head.T, preferred_element_type=jnp.float32) * SOFTMAX_SCALE
            same_doc = doc_blk[:, None] == doc_ids[None, :]
            scores = jnp.where(same_doc, scores, -jnp.inf)
            weights = jax.nn.softmax(scores, axis=-1).astype(jnp.bfloat16).astype(jnp.float32)
            return jnp.dot(weights, value_head, preferred_element_type=jnp.float32)

        context = lax.map(block_attention, (query_blocks, doc_blocks))
        return context.reshape(SEQ_LEN, HEAD_DIM).astype(jnp.bfloat16)

    context_all = lax.map(head_attention, per_head)
    context_all = context_all.transpose(1, 0, 2).reshape(SEQ_LEN, HIDDEN)
    return jnp.dot(context_all, w_out, preferred_element_type=jnp.float32).astype(jnp.bfloat16)
```

```python
import functools

import jax
import jax.numpy as jnp
from jax import lax
from jax.experimental import pallas as pl
from jax.experimental.pallas import tpu as pltpu
from jax.sharding import PartitionSpec as P

HEAD_DIM = 128
SOFTMAX_SCALE = HEAD_DIM ** -0.5
MESH = pl.DeviceIdType.MESH
HW = 3 * HEAD_DIM
BF16 = jnp.bfloat16
F32 = jnp.float32
ANY = pl.BlockSpec(memory_space=pl.ANY)
VM = pl.BlockSpec(memory_space=pltpu.VMEM)
ROWS_MM = 256


def _place(nsp, ntp):
    sp, y = lax.axis_index("sp"), lax.axis_index("tp")
    x, c = sp // 2, sp % 2
    nx = nsp // 2
    xs = [x, lax.rem(x + nx - 1, nx), lax.rem(x + 1, nx), lax.rem(x + 2, nx)]
    ys = [y, lax.rem(y + ntp - 1, ntp), lax.rem(y + 1, ntp), lax.rem(y + 2, ntp)]
    return sp, y, c, xs, ys


def qkv_kernel(nsp, ntp, x_ref, seg_ref, w_ref, qkv_ref, xall, wall, wst, segall,
               acc, xbuf, wbuf, xown, sown, loc, xs_s, xs_r, y_s, y_r, p_s, p_r, w_s, w_r, s_s, s_r):
    sp, y, c, xs, ys = _place(nsp, ntp)
    rows, kcols = x_ref.shape
    krows = w_ref.shape[0]
    half, khalf = rows // 2, krows // 2
    tokens = rows * nsp

    def dev(xi, ci, yi):
        return {"sp": 2 * xi + ci, "tp": yi}

    def rc(src, dst, ss, rs, to):
        return pltpu.make_async_remote_copy(
            src_ref=src, dst_ref=dst, send_sem=ss, recv_sem=rs, device_id=to, device_id_type=MESH)

    own_in = pltpu.make_async_copy(x_ref, xown, loc.at[0])
    own_in.start()

    barrier = pltpu.get_barrier_semaphore()
    greet = []
    for i in (1, 2, 3):
        for ci in (0, 1):
            greet.append(dev(xs[i], ci, y))
    greet.append(dev(xs[0], 1 - c, y))
    greet += [dev(xs[0], c, ys[1]), dev(xs[0], c, ys[2])]
    for d in greet:
        pl.semaphore_signal(barrier, inc=1, device_id=d, device_id_type=MESH)
    pl.semaphore_wait(barrier, len(greet))

    sends = []

    def go(cp):
        cp.start()
        sends.append(cp)

    partner = dev(xs[0], 1 - c, y)
    left, right = (xs[1], c, y), (xs[2], c, y)

    def blk(yi, xi):
        return xall.at[yi, 2 * xi + c]

    go(rc(x_ref, blk(y, xs[0]), xs_s.at[0], xs_r.at[0], dev(*right)))
    go(rc(x_ref, blk(y, xs[0]), xs_s.at[1], xs_r.at[1], dev(*left)))
    go(rc(x_ref, blk(y, xs[0]), y_s.at[0, 0], y_r.at[0, 0], dev(xs[0], c, ys[2])))
    go(rc(x_ref, blk(y, xs[0]), y_s.at[1, 0], y_r.at[1, 0], dev(xs[0], c, ys[1])))
    go(rc(x_ref, blk(y, xs[0]), p_s.at[0, 0], p_r.at[0, 0], partner))
    n = 0
    for i in range(4):
        for ci in (0, 1):
            if i == 0 and ci == 1:
                continue
            cc = (1 - c) if i == 0 else ci
            back = {0: 0, 1: 2, 2: 1, 3: 3}[i]
            go(rc(seg_ref, segall.at[sp], s_s.at[n], s_r.at[back, c], dev(xs[i], cc, y)))
            n += 1

    def wcol(h, j, num):
        return pl.ds(pl.multiple_of((h * nsp + j) * HW, 128), num * HW)

    def w_far(h):
        go(rc(w_ref.at[pl.ds(0, khalf), wcol(h, 2 * xs[3], 2)], wst.at[0, h], w_s.at[h, 0], w_r.at[h, 0], dev(*right)))
        go(rc(w_ref.at[pl.ds(khalf, khalf), wcol(h, 2 * xs[3], 2)], wst.at[1, h], w_s.at[h, 1], w_r.at[h, 1], dev(*left)))

    def w_near(h):
        for ci in (0, 1):
            go(rc(w_ref.at[:, wcol(h, 2 * xs[2] + ci, 1)], wall.at[h, sp], w_s.at[h, 2 + ci], w_r.at[h, 2 + c], dev(xs[2], ci, y)))
            go(rc(w_ref.at[:, wcol(h, 2 * xs[1] + ci, 1)], wall.at[h, sp], w_s.at[h, 4 + ci], w_r.at[h, 4 + c], dev(xs[1], ci, y)))

    def w_pass(h):
        for ci in (0, 1):
            cols = pl.ds(ci * HW, HW)
            go(rc(wst.at[0, h, :, cols], wall.at[h, 2 * xs[1] + c, pl.ds(0, khalf)],
                  w_s.at[h, 6 + ci], w_r.at[h, 6 + c], dev(xs[2], ci, y)))
            go(rc(wst.at[1, h, :, cols], wall.at[h, 2 * xs[2] + c, pl.ds(khalf, khalf)],
                  w_s.at[h, 8 + ci], w_r.at[h, 8 + c], dev(xs[1], ci, y)))

    def w_partner(h):
        go(rc(w_ref.at[:, wcol(h, 2 * xs[0] + 1 - c, 1)], wall.at[h, sp], w_s.at[h, 10], w_r.at[h, 10], partner))

    w_far(0)
    w_partner(0)
    w_partner(1)

    def own(src, via, dst):
        a = pltpu.make_async_copy(src, via, loc.at[5])
        a.start()
        a.wait()
        b = pltpu.make_async_copy(via, dst, loc.at[5])
        b.start()
        b.wait()

    own_in.wait()
    own_out = pltpu.make_async_copy(xown, blk(y, xs[0]), loc.at[0])
    own_out.start()
    for h in (0, 1):
        own(w_ref.at[:, wcol(h, sp, 1)], wbuf.at[h], wall.at[h, sp])
    own(seg_ref, sown, segall.at[sp])

    def wait(dst, sem):
        pltpu.make_async_copy(dst, dst, sem).wait()

    def y_send(i):
        go(rc(blk(y, xs[i]), blk(y, xs[i]), y_s.at[0, i], y_r.at[0, i], dev(xs[0], c, ys[2])))
        go(rc(blk(y, xs[i]), blk(y, xs[i]), y_s.at[1, i], y_r.at[1, i], dev(xs[0], c, ys[1])))

    def to_partner(j, i):
        go(rc(blk(ys[j], xs[i]), blk(ys[j], xs[i]), p_s.at[j, i], p_r.at[j, i], partner))

    wait(blk(y, xs[1]), xs_r.at[0])
    go(rc(blk(y, xs[1]).at[pl.ds(0, half)], blk(y, xs[1]).at[pl.ds(0, half)], xs_s.at[2], xs_r.at[2], dev(*right)))
    wait(blk(y, xs[2]), xs_r.at[1])
    go(rc(blk(y, xs[2]).at[pl.ds(half, half)], blk(y, xs[2]).at[pl.ds(half, half)], xs_s.at[3], xs_r.at[3], dev(*left)))
    w_near(0)
    for i in (1, 2):
        y_send(i)
        to_partner(0, i)

    def y_pass(i):
        wait(blk(ys[1], xs[i]), y_r.at[0, i])
        if i in (0, 3):
            go(rc(blk(ys[1], xs[i]), blk(ys[1], xs[i]), y_s.at[2, i], y_r.at[2, i], dev(xs[0], c, ys[2])))
        to_partner(1, i)
        wait(blk(ys[2], xs[i]), y_r.at[1, i])
        if i in (1, 2):
            go(rc(blk(ys[2], xs[i]), blk(ys[2], xs[i]), y_s.at[2, i], y_r.at[2, i], dev(xs[0], c, ys[1])))
        to_partner(2, i)

    y_pass(0)
    wait(wst.at[0, 0], w_r.at[0, 0])
    wait(wst.at[1, 0], w_r.at[0, 1])
    w_pass(0)
    w_far(1)
    w_near(1)
    wait(blk(y, xs[3]).at[pl.ds(0, half)], xs_r.at[2])
    wait(blk(y, xs[3]).at[pl.ds(half, half)], xs_r.at[3])
    y_send(3)
    to_partner(0, 3)

    acc[...] = jnp.zeros_like(acc)
    y_pass(1)
    y_pass(2)
    y_pass(3)

    def from_partner(j):
        for i in range(4):
            d = xall.at[ys[j], 2 * xs[i] + 1 - c]
            wait(d, p_r.at[j, i])

    def w_wait_near(h):
        for ci in (0, 1):
            wait(wall.at[h, 2 * xs[1] + ci], w_r.at[h, 2 + ci])
            wait(wall.at[h, 2 * xs[2] + ci], w_r.at[h, 4 + ci])

    def w_wait_far(h):
        for ci in (0, 1):
            wait(wall.at[h, 2 * xs[3] + ci, pl.ds(0, khalf)], w_r.at[h, 6 + ci])
            wait(wall.at[h, 2 * xs[3] + ci, pl.ds(khalf, khalf)], w_r.at[h, 8 + ci])

    def run(h, count, src_of):
        def load(i, slot):
            s = src_of(i)
            k, part = s // 2, s % 2
            cols = pl.ds(pl.multiple_of(part * krows, 128), krows)
            xc = [pltpu.make_async_copy(xall.at[k, r, :, cols], xbuf.at[slot, pl.ds(r * rows, rows)], loc.at[1 + slot])
                  for r in range(nsp)]
            wc = pltpu.make_async_copy(wall.at[h, s], wbuf.at[slot], loc.at[3 + slot])
            return xc, wc

        def start(i, slot):
            xc, wc = load(i, slot)
            for cp in xc:
                cp.start()
            wc.start()

        start(0, 0)

        def step(i, carry):
            slot = lax.rem(i, 2)

            @pl.when(i + 1 < count)
            def _():
                start(i + 1, 1 - slot)

            _, wc = load(i, slot)
            pltpu.make_async_copy(xbuf.at[slot], xbuf.at[slot], loc.at[1 + slot]).wait()
            wc.wait()

            def mm(rb, carry):
                r = pl.ds(pl.multiple_of(rb * ROWS_MM, ROWS_MM), ROWS_MM)
                acc[h, r, :] += jnp.dot(xbuf[slot, r, :], wbuf[slot], preferred_element_type=F32)
                return carry

            lax.fori_loop(0, tokens // ROWS_MM, mm, 0)
            return carry

        lax.fori_loop(0, count, step, 0)

    def cast(h):
        def body(rb, carry):
            r = pl.ds(pl.multiple_of(rb * ROWS_MM, ROWS_MM), ROWS_MM)
            qkv_ref[h, r, :] = acc[h, r, :].astype(BF16)
            return carry
        lax.fori_loop(0, tokens // ROWS_MM, body, 0)

    nx = nsp // 2

    own_out.wait()
    for j in (0, 1, 2):
        from_partner(j)
    wait(wall.at[0, 2 * xs[0] + 1 - c], w_r.at[0, 10])
    w_wait_near(0)
    w_wait_far(0)
    run(0, 6, lambda i: 2 * lax.rem(ys[1] + i // 2, ntp) + i % 2)
    for i in range(4):
        wait(blk(ys[3], xs[i]), y_r.at[2, i])
        to_partner(3, i)
    wait(wst.at[0, 1], w_r.at[1, 0])
    wait(wst.at[1, 1], w_r.at[1, 1])
    w_pass(1)
    from_partner(3)
    run(0, 2, lambda i: 2 * ys[3] + i)
    cast(0)
    wait(wall.at[1, 2 * xs[0] + 1 - c], w_r.at[1, 10])
    run(1, 2, lambda i: 2 * xs[0] + i)
    w_wait_near(1)
    run(1, 4, lambda i: 2 * lax.rem(xs[1] + 2 * (i // 2), nx) + i % 2)
    w_wait_far(1)
    run(1, 2, lambda i: 2 * xs[3] + i)
    cast(1)

    for back in (1, 2, 3):
        for ci in (0, 1):
            wait(segall.at[2 * xs[back] + ci], s_r.at[back, ci])
    wait(segall.at[2 * xs[0] + 1 - c], s_r.at[0, 1 - c])
    for cp in sends:
        cp.wait_send()


def qkv_call(nsp, ntp, x, seg, w):
    rows, kcols = x.shape
    krows, ncols = w.shape
    tokens = rows * nsp
    dma = pltpu.SemaphoreType.DMA
    out_shape = (
        jax.ShapeDtypeStruct((2, tokens, HW), BF16),
        jax.ShapeDtypeStruct((ntp, nsp, rows, kcols), BF16),
        jax.ShapeDtypeStruct((2, nsp, krows, HW), BF16),
        jax.ShapeDtypeStruct((2, 2, krows // 2, 2 * HW), BF16),
        jax.ShapeDtypeStruct((nsp, 1, rows), jnp.int32),
    )
    return pl.pallas_call(
        functools.partial(qkv_kernel, nsp, ntp),
        name="qkv",
        out_shape=out_shape,
        in_specs=[ANY, ANY, ANY],
        out_specs=(VM, ANY, ANY, ANY, ANY),
        scratch_shapes=[
            pltpu.VMEM((2, tokens, HW), F32),
            pltpu.VMEM((2, tokens, krows), BF16),
            pltpu.VMEM((2, krows, HW), BF16),
            pltpu.VMEM((rows, kcols), BF16),
            pltpu.VMEM((1, rows), jnp.int32),
            dma((6,)),
            dma((4,)), dma((4,)),
            dma((3, 4)), dma((3, 4)),
            dma((4, 4)), dma((4, 4)),
            dma((2, 11)), dma((2, 11)),
            dma((7,)), dma((4, 2)),
        ],
        compiler_params=pltpu.CompilerParams(
            collective_id=0, has_side_effects=True, vmem_limit_bytes=56 * 1024 * 1024),
    )(x, seg, w)


def attn_kernel(nb, lo_ref, hi_ref, segc_ref, segr_ref, q_ref, k_ref, v_ref, o_ref, s_ref):
    i = pl.program_id(1)
    lo, hi = lo_ref[i], hi_ref[i]
    bq, bk = q_ref.shape[1], s_ref.shape[2]
    segc = segc_ref[...]
    q = q_ref[0]

    def cols(kb):
        return pl.ds(pl.multiple_of(kb * bk, bk), bk)

    def scores(kb, m):
        s = lax.dot_general(q, k_ref[0, cols(kb), :], (((1,), (1,)), ((), ())), preferred_element_type=F32)
        s = jnp.where(segc == segr_ref[:, cols(kb)], s * SOFTMAX_SCALE, -jnp.inf)
        s_ref[kb] = s
        return jnp.maximum(m, jnp.max(s, axis=-1, keepdims=True))

    m = lax.fori_loop(lo, hi, scores, jnp.full((bq, 1), -jnp.inf, F32))

    def expo(kb, l):
        e = jnp.exp(s_ref[kb] - m)
        s_ref[kb] = e
        return l + jnp.sum(e, axis=-1, keepdims=True)

    l = lax.fori_loop(lo, hi, expo, jnp.zeros((bq, 1), F32))
    inv = 1.0 / l

    def values(kb, o):
        p = (s_ref[kb] * inv).astype(BF16)
        return o + jnp.dot(p, v_ref[0, cols(kb), :], preferred_element_type=F32)

    o = lax.fori_loop(lo, hi, values, jnp.zeros((bq, HEAD_DIM), F32))
    o_ref[0] = o.astype(BF16)


def attention(qkv, seg, bq=256, bk=256):
    heads, tokens, _ = qkv.shape
    nq, nb = tokens // bq, tokens // bk
    first, last = seg[::bq], seg[bq - 1::bq]
    lo = jnp.sum((seg[None, :] < first[:, None]).astype(jnp.int32), axis=1) // bk
    hi = (jnp.sum((seg[None, :] <= last[:, None]).astype(jnp.int32), axis=1) + bk - 1) // bk
    grid_spec = pltpu.PrefetchScalarGridSpec(
        num_scalar_prefetch=2,
        grid=(heads, nq),
        in_specs=[
            pl.BlockSpec((bq, 1), lambda h, i, *_: (i, 0)),
            pl.BlockSpec((1, tokens), lambda h, i, *_: (0, 0)),
            pl.BlockSpec((1, bq, HEAD_DIM), lambda h, i, *_: (h, i, 0)),
            pl.BlockSpec((1, tokens, HEAD_DIM), lambda h, i, *_: (h, 0, 1)),
            pl.BlockSpec((1, tokens, HEAD_DIM), lambda h, i, *_: (h, 0, 2)),
        ],
        out_specs=pl.BlockSpec((1, bq, HEAD_DIM), lambda h, i, *_: (h, i, 0)),
        scratch_shapes=[pltpu.VMEM((nb, bq, bk), F32)],
    )
    return pl.pallas_call(
        functools.partial(attn_kernel, nb),
        name="attention",
        out_shape=jax.ShapeDtypeStruct((heads, tokens, HEAD_DIM), BF16),
        grid_spec=grid_spec,
    )(lo, hi, seg[:, None], seg[None, :], qkv, qkv, qkv)


def solution(mesh):
    nsp, ntp = mesh.shape["sp"], mesh.shape["tp"]

    def device_block(x_block, doc_block, wqkv_block, wout_block):
        rows = x_block.shape[0]
        qkv, _, _, _, segall = qkv_call(nsp, ntp, x_block, doc_block.reshape(1, rows), wqkv_block)
        context = attention(qkv, segall.reshape(nsp * rows))
        context = context.reshape(2, nsp, rows, HEAD_DIM)
        context = lax.all_to_all(context, "sp", 1, 1, tiled=False)
        context = context.transpose(2, 0, 1, 3).reshape(rows, 2 * nsp * HEAD_DIM)
        ctx_rows = lax.all_gather(context, "tp", axis=1, tiled=True)
        wout_cols = lax.all_gather(wout_block, "sp", axis=0, tiled=True)
        y_block = jnp.dot(ctx_rows, wout_cols, preferred_element_type=F32).astype(BF16)
        return lax.all_to_all(y_block, "tp", 0, 1, tiled=True)

    return jax.shard_map(
        device_block,
        mesh=mesh,
        in_specs=(P(("dp", "sp"), "tp"), P(("dp", "sp")), P("sp", "tp"), P("sp", "tp")),
        out_specs=P(("dp", "sp", "tp"), None),
        check_vma=False,
    )
```

```python
import functools

import jax
import jax.numpy as jnp
from jax import lax
from jax.experimental import pallas as pl
from jax.experimental.pallas import tpu as pltpu
from jax.sharding import PartitionSpec as P

HEAD_DIM = 128
SOFTMAX_SCALE = HEAD_DIM ** -0.5
MESH = pl.DeviceIdType.MESH
HW = 3 * HEAD_DIM
BF16 = jnp.bfloat16
F32 = jnp.float32
ANY = pl.BlockSpec(memory_space=pl.ANY)
VM = pl.BlockSpec(memory_space=pltpu.VMEM)
ROWS_MM = 256


def _place(nsp, ntp):
    sp, y = lax.axis_index("sp"), lax.axis_index("tp")
    x, c = sp // 2, sp % 2
    nx = nsp // 2
    xs = [x, lax.rem(x + nx - 1, nx), lax.rem(x + 1, nx), lax.rem(x + 2, nx)]
    ys = [y, lax.rem(y + ntp - 1, ntp), lax.rem(y + 1, ntp), lax.rem(y + 2, ntp)]
    return sp, y, c, xs, ys


def qkv_kernel(nsp, ntp, x_ref, seg_ref, w_ref, qkv_ref, xall, wall, wst, segall,
               acc, xbuf, wbuf, xown, sown, loc, xs_s, xs_r, y_s, y_r, p_s, p_r, w_s, w_r, s_s, s_r):
    sp, y, c, xs, ys = _place(nsp, ntp)
    rows, kcols = x_ref.shape
    krows = w_ref.shape[0]
    half, khalf = rows // 2, krows // 2
    tokens = rows * nsp

    def dev(xi, ci, yi):
        return {"sp": 2 * xi + ci, "tp": yi}

    def rc(src, dst, ss, rs, to):
        return pltpu.make_async_remote_copy(
            src_ref=src, dst_ref=dst, send_sem=ss, recv_sem=rs, device_id=to, device_id_type=MESH)

    own_in = pltpu.make_async_copy(x_ref, xown, loc.at[0])
    own_in.start()

    barrier = pltpu.get_barrier_semaphore()
    greet = []
    for i in (1, 2, 3):
        for ci in (0, 1):
            greet.append(dev(xs[i], ci, y))
    greet.append(dev(xs[0], 1 - c, y))
    greet += [dev(xs[0], c, ys[1]), dev(xs[0], c, ys[2])]
    for d in greet:
        pl.semaphore_signal(barrier, inc=1, device_id=d, device_id_type=MESH)
    pl.semaphore_wait(barrier, len(greet))

    sends = []

    def go(cp):
        cp.start()
        sends.append(cp)

    partner = dev(xs[0], 1 - c, y)
    left, right = (xs[1], c, y), (xs[2], c, y)

    def blk(yi, xi):
        return xall.at[yi, 2 * xi + c]

    go(rc(x_ref, blk(y, xs[0]), xs_s.at[0], xs_r.at[0], dev(*right)))
    go(rc(x_ref, blk(y, xs[0]), xs_s.at[1], xs_r.at[1], dev(*left)))
    go(rc(x_ref, blk(y, xs[0]), y_s.at[0, 0], y_r.at[0, 0], dev(xs[0], c, ys[2])))
    go(rc(x_ref, blk(y, xs[0]), y_s.at[1, 0], y_r.at[1, 0], dev(xs[0], c, ys[1])))
    go(rc(x_ref, blk(y, xs[0]), p_s.at[0, 0], p_r.at[0, 0], partner))
    n = 0
    for i in range(4):
        for ci in (0, 1):
            if i == 0 and ci == 1:
                continue
            cc = (1 - c) if i == 0 else ci
            back = {0: 0, 1: 2, 2: 1, 3: 3}[i]
            go(rc(seg_ref, segall.at[sp], s_s.at[n], s_r.at[back, c], dev(xs[i], cc, y)))
            n += 1

    def wcol(h, j, num):
        return pl.ds(pl.multiple_of((h * nsp + j) * HW, 128), num * HW)

    def w_far(h):
        go(rc(w_ref.at[pl.ds(0, khalf), wcol(h, 2 * xs[3], 2)], wst.at[0, h], w_s.at[h, 0], w_r.at[h, 0], dev(*right)))
        go(rc(w_ref.at[pl.ds(khalf, khalf), wcol(h, 2 * xs[3], 2)], wst.at[1, h], w_s.at[h, 1], w_r.at[h, 1], dev(*left)))

    def w_near(h):
        for ci in (0, 1):
            go(rc(w_ref.at[:, wcol(h, 2 * xs[2] + ci, 1)], wall.at[h, sp], w_s.at[h, 2 + ci], w_r.at[h, 2 + c], dev(xs[2], ci, y)))
            go(rc(w_ref.at[:, wcol(h, 2 * xs[1] + ci, 1)], wall.at[h, sp], w_s.at[h, 4 + ci], w_r.at[h, 4 + c], dev(xs[1], ci, y)))

    def w_pass(h):
        for ci in (0, 1):
            cols = pl.ds(ci * HW, HW)
            go(rc(wst.at[0, h, :, cols], wall.at[h, 2 * xs[1] + c, pl.ds(0, khalf)],
                  w_s.at[h, 6 + ci], w_r.at[h, 6 + c], dev(xs[2], ci, y)))
            go(rc(wst.at[1, h, :, cols], wall.at[h, 2 * xs[2] + c, pl.ds(khalf, khalf)],
                  w_s.at[h, 8 + ci], w_r.at[h, 8 + c], dev(xs[1], ci, y)))

    def w_partner(h):
        go(rc(w_ref.at[:, wcol(h, 2 * xs[0] + 1 - c, 1)], wall.at[h, sp], w_s.at[h, 10], w_r.at[h, 10], partner))

    w_far(0)
    w_partner(0)
    w_partner(1)

    def own(src, via, dst):
        a = pltpu.make_async_copy(src, via, loc.at[5])
        a.start()
        a.wait()
        b = pltpu.make_async_copy(via, dst, loc.at[5])
        b.start()
        b.wait()

    own_in.wait()
    own_out = pltpu.make_async_copy(xown, blk(y, xs[0]), loc.at[0])
    own_out.start()
    for h in (0, 1):
        own(w_ref.at[:, wcol(h, sp, 1)], wbuf.at[h], wall.at[h, sp])
    own(seg_ref, sown, segall.at[sp])

    def wait(dst, sem):
        pltpu.make_async_copy(dst, dst, sem).wait()

    def y_send(i):
        go(rc(blk(y, xs[i]), blk(y, xs[i]), y_s.at[0, i], y_r.at[0, i], dev(xs[0], c, ys[2])))
        go(rc(blk(y, xs[i]), blk(y, xs[i]), y_s.at[1, i], y_r.at[1, i], dev(xs[0], c, ys[1])))

    def to_partner(j, i):
        go(rc(blk(ys[j], xs[i]), blk(ys[j], xs[i]), p_s.at[j, i], p_r.at[j, i], partner))

    wait(blk(y, xs[1]), xs_r.at[0])
    go(rc(blk(y, xs[1]).at[pl.ds(0, half)], blk(y, xs[1]).at[pl.ds(0, half)], xs_s.at[2], xs_r.at[2], dev(*right)))
    wait(blk(y, xs[2]), xs_r.at[1])
    go(rc(blk(y, xs[2]).at[pl.ds(half, half)], blk(y, xs[2]).at[pl.ds(half, half)], xs_s.at[3], xs_r.at[3], dev(*left)))
    w_near(0)
    for i in (1, 2):
        y_send(i)
        to_partner(0, i)

    def y_pass(i):
        wait(blk(ys[1], xs[i]), y_r.at[0, i])
        if i in (0, 3):
            go(rc(blk(ys[1], xs[i]), blk(ys[1], xs[i]), y_s.at[2, i], y_r.at[2, i], dev(xs[0], c, ys[2])))
        to_partner(1, i)
        wait(blk(ys[2], xs[i]), y_r.at[1, i])
        if i in (1, 2):
            go(rc(blk(ys[2], xs[i]), blk(ys[2], xs[i]), y_s.at[2, i], y_r.at[2, i], dev(xs[0], c, ys[1])))
        to_partner(2, i)

    y_pass(0)
    wait(wst.at[0, 0], w_r.at[0, 0])
    wait(wst.at[1, 0], w_r.at[0, 1])
    w_pass(0)
    w_far(1)
    w_near(1)
    wait(blk(y, xs[3]).at[pl.ds(0, half)], xs_r.at[2])
    wait(blk(y, xs[3]).at[pl.ds(half, half)], xs_r.at[3])
    y_send(3)
    to_partner(0, 3)

    acc[...] = jnp.zeros_like(acc)
    y_pass(1)
    y_pass(2)
    y_pass(3)

    def from_partner(j):
        for i in range(4):
            d = xall.at[ys[j], 2 * xs[i] + 1 - c]
            wait(d, p_r.at[j, i])

    def w_wait_near(h):
        for ci in (0, 1):
            wait(wall.at[h, 2 * xs[1] + ci], w_r.at[h, 2 + ci])
            wait(wall.at[h, 2 * xs[2] + ci], w_r.at[h, 4 + ci])

    def w_wait_far(h):
        for ci in (0, 1):
            wait(wall.at[h, 2 * xs[3] + ci, pl.ds(0, khalf)], w_r.at[h, 6 + ci])
            wait(wall.at[h, 2 * xs[3] + ci, pl.ds(khalf, khalf)], w_r.at[h, 8 + ci])

    def run(h, count, src_of):
        def w_copy(i, slot):
            return pltpu.make_async_copy(wall.at[h, src_of(i)], wbuf.at[slot], loc.at[3 + slot])

        def start(i, slot):
            s = src_of(i)
            cols = pl.ds(pl.multiple_of((s % 2) * krows, 128), krows)
            for r in range(nsp):
                pltpu.make_async_copy(
                    xall.at[s // 2, r, :, cols], xbuf.at[slot, pl.ds(r * rows, rows)], loc.at[1 + slot]).start()
            w_copy(i, slot).start()

        start(0, 0)

        def step(i, carry):
            slot = lax.rem(i, 2)

            @pl.when(i + 1 < count)
            def _():
                start(i + 1, 1 - slot)

            wait(xbuf.at[slot], loc.at[1 + slot])
            w_copy(i, slot).wait()

            def mm(rb, carry):
                r = pl.ds(pl.multiple_of(rb * ROWS_MM, ROWS_MM), ROWS_MM)
                acc[h, r, :] += jnp.dot(xbuf[slot, r, :], wbuf[slot], preferred_element_type=F32)
                return carry

            lax.fori_loop(0, tokens // ROWS_MM, mm, 0)
            return carry

        lax.fori_loop(0, count, step, 0)

    def cast(h):
        def body(rb, carry):
            r = pl.ds(pl.multiple_of(rb * ROWS_MM, ROWS_MM), ROWS_MM)
            qkv_ref[h, r, :] = acc[h, r, :].astype(BF16)
            return carry
        lax.fori_loop(0, tokens // ROWS_MM, body, 0)

    nx = nsp // 2

    own_out.wait()
    for j in (0, 1, 2):
        from_partner(j)
    wait(wall.at[0, 2 * xs[0] + 1 - c], w_r.at[0, 10])
    w_wait_near(0)
    w_wait_far(0)
    run(0, 6, lambda i: 2 * lax.rem(ys[1] + i // 2, ntp) + i % 2)
    for i in range(4):
        wait(blk(ys[3], xs[i]), y_r.at[2, i])
        to_partner(3, i)
    wait(wst.at[0, 1], w_r.at[1, 0])
    wait(wst.at[1, 1], w_r.at[1, 1])
    w_pass(1)
    from_partner(3)
    run(0, 2, lambda i: 2 * ys[3] + i)
    cast(0)
    wait(wall.at[1, 2 * xs[0] + 1 - c], w_r.at[1, 10])
    run(1, 2, lambda i: 2 * xs[0] + i)
    w_wait_near(1)
    run(1, 4, lambda i: 2 * lax.rem(xs[1] + 2 * (i // 2), nx) + i % 2)
    w_wait_far(1)
    run(1, 2, lambda i: 2 * xs[3] + i)
    cast(1)

    for back in (1, 2, 3):
        for ci in (0, 1):
            wait(segall.at[2 * xs[back] + ci], s_r.at[back, ci])
    wait(segall.at[2 * xs[0] + 1 - c], s_r.at[0, 1 - c])
    for cp in sends:
        cp.wait_send()


def qkv_call(nsp, ntp, x, seg, w):
    rows, kcols = x.shape
    krows, ncols = w.shape
    tokens = rows * nsp
    dma = pltpu.SemaphoreType.DMA
    out_shape = (
        jax.ShapeDtypeStruct((2, tokens, HW), BF16),
        jax.ShapeDtypeStruct((ntp, nsp, rows, kcols), BF16),
        jax.ShapeDtypeStruct((2, nsp, krows, HW), BF16),
        jax.ShapeDtypeStruct((2, 2, krows // 2, 2 * HW), BF16),
        jax.ShapeDtypeStruct((nsp, 1, rows), jnp.int32),
    )
    return pl.pallas_call(
        functools.partial(qkv_kernel, nsp, ntp),
        name="qkv",
        out_shape=out_shape,
        in_specs=[ANY, ANY, ANY],
        out_specs=(VM, ANY, ANY, ANY, ANY),
        scratch_shapes=[
            pltpu.VMEM((2, tokens, HW), F32),
            pltpu.VMEM((2, tokens, krows), BF16),
            pltpu.VMEM((2, krows, HW), BF16),
            pltpu.VMEM((rows, kcols), BF16),
            pltpu.VMEM((1, rows), jnp.int32),
            dma((6,)),
            dma((4,)), dma((4,)),
            dma((3, 4)), dma((3, 4)),
            dma((4, 4)), dma((4, 4)),
            dma((2, 11)), dma((2, 11)),
            dma((7,)), dma((4, 2)),
        ],
        compiler_params=pltpu.CompilerParams(
            collective_id=0, has_side_effects=True, vmem_limit_bytes=56 * 1024 * 1024),
    )(x, seg, w)


def attn_kernel(nb, lo_ref, hi_ref, segc_ref, segr_ref, q_ref, k_ref, v_ref, o_ref, s_ref):
    i = pl.program_id(1)
    lo, hi = lo_ref[i], hi_ref[i]
    bq, bk = q_ref.shape[1], s_ref.shape[2]
    segc = segc_ref[...]
    q = q_ref[0]

    def cols(kb):
        return pl.ds(pl.multiple_of(kb * bk, bk), bk)

    def scores(kb, m):
        s = lax.dot_general(q, k_ref[0, cols(kb), :], (((1,), (1,)), ((), ())), preferred_element_type=F32)
        s = jnp.where(segc == segr_ref[:, cols(kb)], s * SOFTMAX_SCALE, -jnp.inf)
        s_ref[kb] = s
        return jnp.maximum(m, jnp.max(s, axis=-1, keepdims=True))

    m = lax.fori_loop(lo, hi, scores, jnp.full((bq, 1), -jnp.inf, F32))

    def expo(kb, l):
        e = jnp.exp(s_ref[kb] - m)
        s_ref[kb] = e
        return l + jnp.sum(e, axis=-1, keepdims=True)

    l = lax.fori_loop(lo, hi, expo, jnp.zeros((bq, 1), F32))
    inv = 1.0 / l

    def values(kb, o):
        p = (s_ref[kb] * inv).astype(BF16)
        return o + jnp.dot(p, v_ref[0, cols(kb), :], preferred_element_type=F32)

    o = lax.fori_loop(lo, hi, values, jnp.zeros((bq, HEAD_DIM), F32))
    o_ref[...] = o.astype(BF16)


def attention(qkv, seg, bq=256, bk=256):
    heads, tokens, _ = qkv.shape
    nq, nb = tokens // bq, tokens // bk
    first, last = seg[::bq], seg[bq - 1::bq]
    lo = jnp.sum((seg[None, :] < first[:, None]).astype(jnp.int32), axis=1) // bk
    hi = (jnp.sum((seg[None, :] <= last[:, None]).astype(jnp.int32), axis=1) + bk - 1) // bk
    grid_spec = pltpu.PrefetchScalarGridSpec(
        num_scalar_prefetch=2,
        grid=(heads, nq),
        in_specs=[
            pl.BlockSpec((bq, 1), lambda h, i, *_: (i, 0)),
            pl.BlockSpec((1, tokens), lambda h, i, *_: (0, 0)),
            pl.BlockSpec((1, bq, HEAD_DIM), lambda h, i, *_: (h, i, 0)),
            pl.BlockSpec((1, tokens, HEAD_DIM), lambda h, i, *_: (h, 0, 1)),
            pl.BlockSpec((1, tokens, HEAD_DIM), lambda h, i, *_: (h, 0, 2)),
        ],
        out_specs=pl.BlockSpec((bq, HEAD_DIM), lambda h, i, *_: (i, h)),
        scratch_shapes=[pltpu.VMEM((nb, bq, bk), F32)],
    )
    return pl.pallas_call(
        functools.partial(attn_kernel, nb),
        name="attention",
        out_shape=jax.ShapeDtypeStruct((tokens, heads * HEAD_DIM), BF16),
        grid_spec=grid_spec,
    )(lo, hi, seg[:, None], seg[None, :], qkv, qkv, qkv)


def out_kernel(nsp, ntp, o_ref, w_ref, y_ref, og, s1, wo, part, far, near, ybuf,
               loc, w_s, w_r, a_s, a_r, b_s, b_r, g_s, g_r, p_s, p_r, f_s, f_r, n_s, n_r, y_s, y_r):
    sp, y, c, xs, ys = _place(nsp, ntp)
    x = xs[0]
    nx = nsp // 2
    tokens, width = o_ref.shape
    quarter = tokens // nx
    sub = quarter // ntp
    kw = nx * width
    ncol = wo.shape[1]
    nh = ncol // 2
    out_rows = y_ref.shape[0]

    def dev(xi, ci, yi):
        return {"sp": 2 * xi + ci, "tp": yi}

    def rc(src, dst, ss, rs, to):
        return pltpu.make_async_remote_copy(
            src_ref=src, dst_ref=dst, send_sem=ss, recv_sem=rs, device_id=to, device_id_type=MESH)

    def wait(dst, sem):
        pltpu.make_async_copy(dst, dst, sem).wait()

    def wo_rows(j, hc):
        return pl.ds(pl.multiple_of((j % 2) * kw + (j // 2) * width + hc * HEAD_DIM, 128), HEAD_DIM)

    def w_cols(half):
        return pl.ds(pl.multiple_of(half * ncol, 128), ncol)

    for j in range(nsp):
        pltpu.make_async_copy(w_ref.at[pl.ds(j * HEAD_DIM, HEAD_DIM), w_cols(c)], wo.at[wo_rows(j, c)], loc.at[0]).start()

    barrier = pltpu.get_barrier_semaphore()
    greet = [dev(xs[i], c, y) for i in (1, 2, 3)]
    greet += [dev(x, ci, ys[i]) for i in (1, 2, 3) for ci in (0, 1)]
    greet.append(dev(x, 1 - c, y))
    for d in greet:
        pl.semaphore_signal(barrier, inc=1, device_id=d, device_id_type=MESH)
    pl.semaphore_wait(barrier, len(greet))

    sends = []

    def go(cp):
        cp.start()
        sends.append(cp)

    partner = dev(x, 1 - c, y)

    def quarter_of(q, g):
        return lax.rem(g + (2, 1, nx - 1, 0)[q], nx)

    def o_rows(q, r):
        return o_ref.at[pl.ds(pl.multiple_of(quarter_of(q, y) * quarter + r * sub, sub), sub)]

    def r_rows(r):
        return pl.ds(pl.multiple_of(r * sub, sub), sub)

    def cell(q, r, xi):
        return og.at[q, r_rows(r), pl.ds(pl.multiple_of(c * kw + xi * width, 128), width)]

    diagonal = x == y

    def stage1(q):
        for i in (1, 2, 3):
            r = ys[i]

            @pl.when(diagonal)
            def _():
                rc(o_rows(q, r), cell(q, r, x), a_s.at[q, i], a_r.at[q, y], dev(x, c, r)).start()

            @pl.when(jnp.logical_not(diagonal))
            def _():
                rc(o_rows(q, r), s1.at[q, y], a_s.at[q, i], a_r.at[q, y], dev(x, c, r)).start()

        @pl.when(diagonal)
        def _():
            pltpu.make_async_copy(o_rows(q, y), cell(q, y, x), loc.at[1 + q]).start()

    def stage2(q):
        @pl.when(jnp.logical_not(diagonal))
        def _():
            rc(o_rows(q, y), cell(q, y, x), b_s.at[q, 0], b_r.at[q, x], dev(y, c, y)).start()

        for i in (1, 2, 3):
            g = ys[i]
            wait(s1.at[q, g], a_r.at[q, g])

            @pl.when(g != x)
            def _():
                rc(s1.at[q, g], cell(q, y, x), b_s.at[q, i], b_r.at[q, x], dev(g, c, y)).start()

    def block(q, r, core):
        return og.at[q, r_rows(r), pl.ds(pl.multiple_of(core * kw, 128), kw)]

    def stage3(q):
        for i in (1, 2, 3):
            wait(cell(q, y, xs[i]), b_r.at[q, xs[i]])

        @pl.when(diagonal)
        def _():
            wait(cell(q, y, x), loc.at[1 + q])

        b = block(q, y, c)
        go(rc(b, b, p_s.at[q, 0], p_r.at[q, 0], partner))
        go(rc(b, b, g_s.at[q, 0], g_r.at[q, 0], dev(x, c, ys[2])))
        go(rc(b, b, g_s.at[q, 1], g_r.at[q, 1], dev(x, c, ys[1])))

    hs = sub // 2

    def pass_on(q):
        d, u = block(q, ys[1], c), block(q, ys[2], c)
        top, bottom = pl.ds(0, hs), pl.ds(hs, hs)
        wait(d, g_r.at[q, 0])
        go(rc(d.at[top], d.at[top], g_s.at[q, 2], g_r.at[q, 2], dev(x, c, ys[2])))
        go(rc(d, d, p_s.at[q, 1], p_r.at[q, 1], partner))
        wait(u, g_r.at[q, 1])
        go(rc(u.at[bottom], u.at[bottom], g_s.at[q, 3], g_r.at[q, 3], dev(x, c, ys[1])))
        go(rc(u, u, p_s.at[q, 2], p_r.at[q, 2], partner))

    def far_block(q):
        b = block(q, ys[3], c)
        wait(b.at[pl.ds(0, hs)], g_r.at[q, 2])
        wait(b.at[pl.ds(hs, hs)], g_r.at[q, 3])
        go(rc(b, b, p_s.at[q, 3], p_r.at[q, 3], partner))

    def from_partner(q, i):
        wait(block(q, ys[i], 1 - c), p_r.at[q, i])

    nt = 256

    def mm(q, start, count):
        rows = pl.ds(start, count)

        def body(n, carry):
            cols = pl.ds(pl.multiple_of(n * nt, nt), nt)
            part[q, rows, cols] = jnp.dot(og[q, rows, :], wo[:, cols], preferred_element_type=F32)
            return carry

        lax.fori_loop(0, ncol // nt, body, 0)

    left, right = dev(xs[1], c, y), dev(xs[2], c, y)
    cl, cr = pl.ds(0, nh), pl.ds(nh, nh)

    def send_far(i):
        r = r_rows(ys[i])
        go(rc(part.at[0, r, cl], far.at[0, r], f_s.at[0, i], f_r.at[0, i], right))
        go(rc(part.at[0, r, cr], far.at[1, r], f_s.at[1, i], f_r.at[1, i], left))

    def send_near_first(q, i):
        r = r_rows(ys[i])
        if q == 1:
            go(rc(part.at[1, r, cr], near.at[0, r, cr], n_s.at[0, 0, i], n_r.at[0, 0, i], right))
        else:
            go(rc(part.at[2, r, cl], near.at[1, r, cl], n_s.at[1, 0, i], n_r.at[1, 0, i], left))

    def send_near_second(i):
        r = r_rows(ys[i])
        wait(far.at[0, r], f_r.at[0, i])
        part[1, r, cl] += far[0, r, :]
        go(rc(part.at[1, r, cl], near.at[0, r, cl], n_s.at[0, 1, i], n_r.at[0, 1, i], right))
        wait(far.at[1, r], f_r.at[1, i])
        part[2, r, cr] += far[1, r, :]
        go(rc(part.at[2, r, cr], near.at[1, r, cr], n_s.at[1, 1, i], n_r.at[1, 1, i], left))

    stage1(0)
    for j in range(nsp):
        go(rc(w_ref.at[pl.ds(j * HEAD_DIM, HEAD_DIM), w_cols(1 - c)], wo.at[wo_rows(j, c)], w_s.at[j], w_r.at[0], partner))
    stage1(1)
    stage2(0)
    stage3(0)
    stage1(2)
    stage1(3)
    stage2(1)
    half_w = wo.at[pl.ds(0, nsp * HEAD_DIM)]
    wait(half_w, loc.at[0])
    wait(half_w, w_r.at[0])

    def start_of(i):
        return pl.multiple_of(ys[i] * sub, sub)

    from_partner(0, 0)
    mm(0, start_of(0), sub)
    send_far(0)
    pass_on(0)
    stage3(1)
    for i in (1, 2):
        from_partner(0, i)
        mm(0, start_of(i), sub)
        send_far(i)
    stage2(2)
    far_block(0)
    from_partner(0, 3)
    mm(0, start_of(3), sub)
    send_far(3)
    pass_on(1)
    stage3(2)
    stage2(3)
    far_block(1)
    for i in range(4):
        from_partner(1, i)
    mm(1, 0, quarter)
    for i in range(4):
        send_near_first(1, i)
    pass_on(2)
    stage3(3)
    far_block(2)
    for i in range(4):
        from_partner(2, i)
    mm(2, 0, quarter)
    for i in range(4):
        send_near_first(2, i)
    for i in range(3):
        send_near_second(i)
    pass_on(3)
    far_block(3)
    send_near_second(3)
    for i in range(4):
        from_partner(3, i)
    mm(3, 0, quarter)

    ocols = pl.ds(pl.multiple_of((2 * y + c) * ncol, 128), ncol)
    per = sub // out_rows

    def owner(i, u):
        b = ys[i] * per + u
        return b // ntp, lax.rem(b, ntp)

    def ysrc(i, u):
        return ybuf.at[pl.ds(pl.multiple_of((ys[i] * per + u) * out_rows, out_rows), out_rows)]

    def to_owner(i, u):
        ci, yi = owner(i, u)
        mine = jnp.logical_and(ci == c, yi == y)
        remote = rc(ysrc(i, u), y_ref.at[:, ocols], y_s.at[i, u], y_r.at[y, c], dev(x, ci, yi))
        local = pltpu.make_async_copy(ysrc(i, u), y_ref.at[:, ocols], y_s.at[i, u])
        return mine, remote, local

    for i in range(4):
        r = r_rows(ys[i])
        wait(near.at[0, r, cr], n_r.at[0, 0, i])
        wait(near.at[1, r, cl], n_r.at[1, 0, i])
        wait(near.at[0, r, cl], n_r.at[0, 1, i])
        wait(near.at[1, r, cr], n_r.at[1, 1, i])
        ybuf[r, :] = (part[3, r, :] + near[0, r, :] + near[1, r, :]).astype(BF16)
        for u in range(per):
            mine, remote, local = to_owner(i, u)

            @pl.when(mine)
            def _():
                local.start()

            @pl.when(jnp.logical_not(mine))
            def _():
                remote.start()

    for i in range(4):
        for ci in (0, 1):
            if i == 0:
                continue
            wait(y_ref.at[:, pl.ds(pl.multiple_of((2 * ys[i] + ci) * ncol, 128), ncol)], y_r.at[ys[i], ci])
    wait(y_ref.at[:, pl.ds(pl.multiple_of((2 * y + 1 - c) * ncol, 128), ncol)], y_r.at[y, 1 - c])
    for i in range(4):
        for u in range(per):
            mine, remote, local = to_owner(i, u)

            @pl.when(mine)
            def _():
                local.wait()

            @pl.when(jnp.logical_not(mine))
            def _():
                remote.wait_send()
    for cp in sends:
        cp.wait_send()
    for q in range(4):
        for i in (1, 2, 3):
            rc(o_rows(q, ys[i]), s1.at[q, y], a_s.at[q, i], a_r.at[q, y], dev(x, c, ys[i])).wait_send()

            @pl.when(ys[i] != x)
            def _():
                rc(s1.at[q, ys[i]], cell(q, y, x), b_s.at[q, i], b_r.at[q, x], dev(ys[i], c, y)).wait_send()

        @pl.when(jnp.logical_not(diagonal))
        def _():
            rc(o_rows(q, y), cell(q, y, x), b_s.at[q, 0], b_r.at[q, x], dev(y, c, y)).wait_send()


def out_call(nsp, ntp, o, w):
    tokens, width = o.shape
    krows, wcols = w.shape
    nx = nsp // 2
    quarter, ncol = tokens // nx, wcols // 2
    sub = quarter // ntp
    dma = pltpu.SemaphoreType.DMA
    return pl.pallas_call(
        functools.partial(out_kernel, nsp, ntp),
        name="out",
        out_shape=jax.ShapeDtypeStruct((tokens // (nsp * ntp), ntp * wcols), BF16),
        in_specs=[ANY, ANY],
        out_specs=ANY,
        scratch_shapes=[
            pltpu.VMEM((4, quarter, nsp * width), BF16),
            pltpu.VMEM((4, ntp, sub, width), BF16),
            pltpu.VMEM((2 * krows, ncol), BF16),
            pltpu.VMEM((4, quarter, ncol), F32),
            pltpu.VMEM((2, quarter, ncol // 2), F32),
            pltpu.VMEM((2, quarter, ncol), F32),
            pltpu.VMEM((quarter, ncol), BF16),
            dma((5,)),
            dma((nsp,)), dma((1,)),
            dma((4, 4)), dma((4, 4)),
            dma((4, 4)), dma((4, 4)),
            dma((4, 4)), dma((4, 4)),
            dma((4, 4)), dma((4, 4)),
            dma((2, 4)), dma((2, 4)),
            dma((2, 2, 4)), dma((2, 2, 4)),
            dma((4, 2)), dma((4, 2)),
        ],
        compiler_params=pltpu.CompilerParams(
            collective_id=1, has_side_effects=True, vmem_limit_bytes=60 * 1024 * 1024),
    )(o, w)


def solution(mesh):
    nsp, ntp = mesh.shape["sp"], mesh.shape["tp"]

    def device_block(x_block, doc_block, wqkv_block, wout_block):
        rows = x_block.shape[0]
        qkv, _, _, _, segall = qkv_call(nsp, ntp, x_block, doc_block.reshape(1, rows), wqkv_block)
        context = attention(qkv, segall.reshape(nsp * rows))
        return out_call(nsp, ntp, context, wout_block)

    return jax.shard_map(
        device_block,
        mesh=mesh,
        in_specs=(P(("dp", "sp"), "tp"), P(("dp", "sp")), P("sp", "tp"), P("sp", "tp")),
        out_specs=P(("dp", "sp", "tp"), None),
        check_vma=False,
    )
```

```python
import functools

import jax
import jax.numpy as jnp
from jax import lax
from jax.experimental import pallas as pl
from jax.experimental.pallas import tpu as pltpu
from jax.sharding import PartitionSpec as P

HEAD_DIM = 128
SOFTMAX_SCALE = HEAD_DIM ** -0.5
MESH = pl.DeviceIdType.MESH
HW = 3 * HEAD_DIM
BF16 = jnp.bfloat16
F32 = jnp.float32
ANY = pl.BlockSpec(memory_space=pl.ANY)
VM = pl.BlockSpec(memory_space=pltpu.VMEM)
ROWS_MM = 256


def _place(nsp, ntp):
    sp, y = lax.axis_index("sp"), lax.axis_index("tp")
    x, c = sp // 2, sp % 2
    nx = nsp // 2
    xs = [x, lax.rem(x + nx - 1, nx), lax.rem(x + 1, nx), lax.rem(x + 2, nx)]
    ys = [y, lax.rem(y + ntp - 1, ntp), lax.rem(y + 1, ntp), lax.rem(y + 2, ntp)]
    return sp, y, c, xs, ys


def qkv_kernel(nsp, ntp, x_ref, seg_ref, w_ref, qkv_ref, xall, wall, wst, segall,
               acc, xbuf, wbuf, xown, sown, loc, xs_s, xs_r, y_s, y_r, p_s, p_r, w_s, w_r, s_s, s_r):
    sp, y, c, xs, ys = _place(nsp, ntp)
    rows, kcols = x_ref.shape
    krows = w_ref.shape[0]
    half, khalf = rows // 2, krows // 2
    tokens = rows * nsp

    def dev(xi, ci, yi):
        return {"sp": 2 * xi + ci, "tp": yi}

    def rc(src, dst, ss, rs, to):
        return pltpu.make_async_remote_copy(
            src_ref=src, dst_ref=dst, send_sem=ss, recv_sem=rs, device_id=to, device_id_type=MESH)

    own_in = pltpu.make_async_copy(x_ref, xown, loc.at[0])
    own_in.start()

    barrier = pltpu.get_barrier_semaphore()
    greet = []
    for i in (1, 2, 3):
        for ci in (0, 1):
            greet.append(dev(xs[i], ci, y))
    greet.append(dev(xs[0], 1 - c, y))
    greet += [dev(xs[0], c, ys[1]), dev(xs[0], c, ys[2])]
    for d in greet:
        pl.semaphore_signal(barrier, inc=1, device_id=d, device_id_type=MESH)
    pl.semaphore_wait(barrier, len(greet))

    sends = []

    def go(cp):
        cp.start()
        sends.append(cp)

    partner = dev(xs[0], 1 - c, y)
    left, right = (xs[1], c, y), (xs[2], c, y)

    def blk(yi, xi):
        return xall.at[yi, 2 * xi + c]

    go(rc(x_ref, blk(y, xs[0]), xs_s.at[0], xs_r.at[0], dev(*right)))
    go(rc(x_ref, blk(y, xs[0]), xs_s.at[1], xs_r.at[1], dev(*left)))
    go(rc(x_ref, blk(y, xs[0]), y_s.at[0, 0], y_r.at[0, 0], dev(xs[0], c, ys[2])))
    go(rc(x_ref, blk(y, xs[0]), y_s.at[1, 0], y_r.at[1, 0], dev(xs[0], c, ys[1])))
    go(rc(x_ref, blk(y, xs[0]), p_s.at[0, 0], p_r.at[0, 0], partner))
    n = 0
    for i in range(4):
        for ci in (0, 1):
            if i == 0 and ci == 1:
                continue
            cc = (1 - c) if i == 0 else ci
            back = {0: 0, 1: 2, 2: 1, 3: 3}[i]
            go(rc(seg_ref, segall.at[sp], s_s.at[n], s_r.at[back, c], dev(xs[i], cc, y)))
            n += 1

    def wcol(h, j, num):
        return pl.ds(pl.multiple_of((h * nsp + j) * HW, 128), num * HW)

    def w_far(h):
        go(rc(w_ref.at[pl.ds(0, khalf), wcol(h, 2 * xs[3], 2)], wst.at[0, h], w_s.at[h, 0], w_r.at[h, 0], dev(*right)))
        go(rc(w_ref.at[pl.ds(khalf, khalf), wcol(h, 2 * xs[3], 2)], wst.at[1, h], w_s.at[h, 1], w_r.at[h, 1], dev(*left)))

    def w_near(h):
        for ci in (0, 1):
            go(rc(w_ref.at[:, wcol(h, 2 * xs[2] + ci, 1)], wall.at[h, sp], w_s.at[h, 2 + ci], w_r.at[h, 2 + c], dev(xs[2], ci, y)))
            go(rc(w_ref.at[:, wcol(h, 2 * xs[1] + ci, 1)], wall.at[h, sp], w_s.at[h, 4 + ci], w_r.at[h, 4 + c], dev(xs[1], ci, y)))

    def w_pass(h):
        for ci in (0, 1):
            cols = pl.ds(ci * HW, HW)
            go(rc(wst.at[0, h, :, cols], wall.at[h, 2 * xs[1] + c, pl.ds(0, khalf)],
                  w_s.at[h, 6 + ci], w_r.at[h, 6 + c], dev(xs[2], ci, y)))
            go(rc(wst.at[1, h, :, cols], wall.at[h, 2 * xs[2] + c, pl.ds(khalf, khalf)],
                  w_s.at[h, 8 + ci], w_r.at[h, 8 + c], dev(xs[1], ci, y)))

    def w_partner(h):
        go(rc(w_ref.at[:, wcol(h, 2 * xs[0] + 1 - c, 1)], wall.at[h, sp], w_s.at[h, 10], w_r.at[h, 10], partner))

    w_far(0)
    w_partner(0)
    w_partner(1)

    def own(src, via, dst):
        a = pltpu.make_async_copy(src, via, loc.at[5])
        a.start()
        a.wait()
        b = pltpu.make_async_copy(via, dst, loc.at[5])
        b.start()
        b.wait()

    own_in.wait()
    own_out = pltpu.make_async_copy(xown, blk(y, xs[0]), loc.at[0])
    own_out.start()
    for h in (0, 1):
        own(w_ref.at[:, wcol(h, sp, 1)], wbuf.at[h], wall.at[h, sp])
    own(seg_ref, sown, segall.at[sp])

    def wait(dst, sem):
        pltpu.make_async_copy(dst, dst, sem).wait()

    def y_send(i):
        go(rc(blk(y, xs[i]), blk(y, xs[i]), y_s.at[0, i], y_r.at[0, i], dev(xs[0], c, ys[2])))
        go(rc(blk(y, xs[i]), blk(y, xs[i]), y_s.at[1, i], y_r.at[1, i], dev(xs[0], c, ys[1])))

    def to_partner(j, i):
        go(rc(blk(ys[j], xs[i]), blk(ys[j], xs[i]), p_s.at[j, i], p_r.at[j, i], partner))

    wait(blk(y, xs[1]), xs_r.at[0])
    go(rc(blk(y, xs[1]).at[pl.ds(0, half)], blk(y, xs[1]).at[pl.ds(0, half)], xs_s.at[2], xs_r.at[2], dev(*right)))
    wait(blk(y, xs[2]), xs_r.at[1])
    go(rc(blk(y, xs[2]).at[pl.ds(half, half)], blk(y, xs[2]).at[pl.ds(half, half)], xs_s.at[3], xs_r.at[3], dev(*left)))
    w_near(0)
    for i in (1, 2):
        y_send(i)
        to_partner(0, i)

    def y_pass(i):
        wait(blk(ys[1], xs[i]), y_r.at[0, i])
        if i in (0, 3):
            go(rc(blk(ys[1], xs[i]), blk(ys[1], xs[i]), y_s.at[2, i], y_r.at[2, i], dev(xs[0], c, ys[2])))
        to_partner(1, i)
        wait(blk(ys[2], xs[i]), y_r.at[1, i])
        if i in (1, 2):
            go(rc(blk(ys[2], xs[i]), blk(ys[2], xs[i]), y_s.at[2, i], y_r.at[2, i], dev(xs[0], c, ys[1])))
        to_partner(2, i)

    y_pass(0)
    wait(wst.at[0, 0], w_r.at[0, 0])
    wait(wst.at[1, 0], w_r.at[0, 1])
    w_pass(0)
    w_far(1)
    w_near(1)
    wait(blk(y, xs[3]).at[pl.ds(0, half)], xs_r.at[2])
    wait(blk(y, xs[3]).at[pl.ds(half, half)], xs_r.at[3])
    y_send(3)
    to_partner(0, 3)

    acc[...] = jnp.zeros_like(acc)
    y_pass(1)
    y_pass(2)
    y_pass(3)

    def from_partner(j):
        for i in range(4):
            d = xall.at[ys[j], 2 * xs[i] + 1 - c]
            wait(d, p_r.at[j, i])

    def w_wait_near(h):
        for ci in (0, 1):
            wait(wall.at[h, 2 * xs[1] + ci], w_r.at[h, 2 + ci])
            wait(wall.at[h, 2 * xs[2] + ci], w_r.at[h, 4 + ci])

    def w_wait_far(h):
        for ci in (0, 1):
            wait(wall.at[h, 2 * xs[3] + ci, pl.ds(0, khalf)], w_r.at[h, 6 + ci])
            wait(wall.at[h, 2 * xs[3] + ci, pl.ds(khalf, khalf)], w_r.at[h, 8 + ci])

    def run(h, count, src_of):
        def w_copy(i, slot):
            return pltpu.make_async_copy(wall.at[h, src_of(i)], wbuf.at[slot], loc.at[3 + slot])

        def start(i, slot):
            s = src_of(i)
            cols = pl.ds(pl.multiple_of((s % 2) * krows, 128), krows)
            for r in range(nsp):
                pltpu.make_async_copy(
                    xall.at[s // 2, r, :, cols], xbuf.at[slot, pl.ds(r * rows, rows)], loc.at[1 + slot]).start()
            w_copy(i, slot).start()

        start(0, 0)

        def step(i, carry):
            slot = lax.rem(i, 2)

            @pl.when(i + 1 < count)
            def _():
                start(i + 1, 1 - slot)

            wait(xbuf.at[slot], loc.at[1 + slot])
            w_copy(i, slot).wait()

            def mm(rb, carry):
                r = pl.ds(pl.multiple_of(rb * ROWS_MM, ROWS_MM), ROWS_MM)
                acc[h, r, :] += jnp.dot(xbuf[slot, r, :], wbuf[slot], preferred_element_type=F32)
                return carry

            lax.fori_loop(0, tokens // ROWS_MM, mm, 0)
            return carry

        lax.fori_loop(0, count, step, 0)

    def cast(h):
        def body(rb, carry):
            r = pl.ds(pl.multiple_of(rb * ROWS_MM, ROWS_MM), ROWS_MM)
            qkv_ref[h, r, :] = acc[h, r, :].astype(BF16)
            return carry
        lax.fori_loop(0, tokens // ROWS_MM, body, 0)

    nx = nsp // 2

    own_out.wait()
    for j in (0, 1, 2):
        from_partner(j)
    wait(wall.at[0, 2 * xs[0] + 1 - c], w_r.at[0, 10])
    w_wait_near(0)
    w_wait_far(0)
    run(0, 6, lambda i: 2 * lax.rem(ys[1] + i // 2, ntp) + i % 2)
    for i in range(4):
        wait(blk(ys[3], xs[i]), y_r.at[2, i])
        to_partner(3, i)
    wait(wst.at[0, 1], w_r.at[1, 0])
    wait(wst.at[1, 1], w_r.at[1, 1])
    w_pass(1)
    from_partner(3)
    run(0, 2, lambda i: 2 * ys[3] + i)
    cast(0)
    wait(wall.at[1, 2 * xs[0] + 1 - c], w_r.at[1, 10])
    run(1, 2, lambda i: 2 * xs[0] + i)
    w_wait_near(1)
    run(1, 4, lambda i: 2 * lax.rem(xs[1] + 2 * (i // 2), nx) + i % 2)
    w_wait_far(1)
    run(1, 2, lambda i: 2 * xs[3] + i)
    cast(1)

    for back in (1, 2, 3):
        for ci in (0, 1):
            wait(segall.at[2 * xs[back] + ci], s_r.at[back, ci])
    wait(segall.at[2 * xs[0] + 1 - c], s_r.at[0, 1 - c])
    for cp in sends:
        cp.wait_send()


def qkv_call(nsp, ntp, x, seg, w):
    rows, kcols = x.shape
    krows, ncols = w.shape
    tokens = rows * nsp
    dma = pltpu.SemaphoreType.DMA
    out_shape = (
        jax.ShapeDtypeStruct((2, tokens, HW), BF16),
        jax.ShapeDtypeStruct((ntp, nsp, rows, kcols), BF16),
        jax.ShapeDtypeStruct((2, nsp, krows, HW), BF16),
        jax.ShapeDtypeStruct((2, 2, krows // 2, 2 * HW), BF16),
        jax.ShapeDtypeStruct((nsp, 1, rows), jnp.int32),
    )
    return pl.pallas_call(
        functools.partial(qkv_kernel, nsp, ntp),
        name="qkv",
        out_shape=out_shape,
        in_specs=[ANY, ANY, ANY],
        out_specs=(VM, ANY, ANY, ANY, ANY),
        scratch_shapes=[
            pltpu.VMEM((2, tokens, HW), F32),
            pltpu.VMEM((2, tokens, krows), BF16),
            pltpu.VMEM((2, krows, HW), BF16),
            pltpu.VMEM((rows, kcols), BF16),
            pltpu.VMEM((1, rows), jnp.int32),
            dma((6,)),
            dma((4,)), dma((4,)),
            dma((3, 4)), dma((3, 4)),
            dma((4, 4)), dma((4, 4)),
            dma((2, 11)), dma((2, 11)),
            dma((7,)), dma((4, 2)),
        ],
        compiler_params=pltpu.CompilerParams(
            collective_id=0, has_side_effects=True, vmem_limit_bytes=56 * 1024 * 1024),
    )(x, seg, w)


EXP_SCALE = SOFTMAX_SCALE * 1.4426950408889634


def score_rows(q, k_ref, h, ids, seg_ref, s_ref, chunk=512):
    tokens = k_ref.shape[1]
    width = seg_ref.shape[2]
    top = None
    for n in range(0, tokens, chunk):
        keys = k_ref[h, n:n + chunk, HEAD_DIM:2 * HEAD_DIM]
        s = lax.dot_general(q, keys, (((1,), (1,)), ((), ())), preferred_element_type=F32)
        for g in range(0, chunk, HEAD_DIM):
            at = n + g
            key_ids = seg_ref[at // width, :, at % width:at % width + HEAD_DIM]
            part = jnp.where(ids == key_ids, s[:, g:g + HEAD_DIM], -jnp.inf)
            s_ref[:, at:at + HEAD_DIM] = part
            top = part if top is None else jnp.maximum(top, part)
    return jnp.max(top, axis=-1, keepdims=True)


def exp_rows(s_ref, top):
    total = None
    for g in range(0, s_ref.shape[1], HEAD_DIM):
        e = jnp.exp2((s_ref[:, g:g + HEAD_DIM] - top) * EXP_SCALE)
        s_ref[:, g:g + HEAD_DIM] = e
        total = e if total is None else total + e
    return 1.0 / jnp.sum(total, axis=-1, keepdims=True)


def value_rows(s_ref, inv, v_ref, h, chunk=512):
    o = None
    for n in range(0, s_ref.shape[1], chunk):
        p = (s_ref[:, n:n + chunk] * inv).astype(BF16)
        d = jnp.dot(p, v_ref[h, n:n + chunk, 2 * HEAD_DIM:], preferred_element_type=F32)
        o = d if o is None else o + d
    return o


def out_kernel(nsp, ntp, qkv_ref, seg_ref, w_ref, y_ref, o_ref, sc0, sc1, og, s1, wo, part, far, near, ybuf,
               loc, w_s, w_r, a_s, a_r, b_s, b_r, g_s, g_r, p_s, p_r, f_s, f_r, n_s, n_r, y_s, y_r):
    sp, y, c, xs, ys = _place(nsp, ntp)
    x = xs[0]
    nx = nsp // 2
    tokens, width = o_ref.shape
    bq = seg_ref.shape[2]
    quarter = tokens // nx
    sub = quarter // ntp
    kw = nx * width
    ncol = wo.shape[1]
    nh = ncol // 2
    out_rows = y_ref.shape[0]

    def dev(xi, ci, yi):
        return {"sp": 2 * xi + ci, "tp": yi}

    def rc(src, dst, ss, rs, to):
        return pltpu.make_async_remote_copy(
            src_ref=src, dst_ref=dst, send_sem=ss, recv_sem=rs, device_id=to, device_id_type=MESH)

    def wait(dst, sem):
        pltpu.make_async_copy(dst, dst, sem).wait()

    def wo_rows(j, hc):
        return pl.ds(pl.multiple_of((j % 2) * kw + (j // 2) * width + hc * HEAD_DIM, 128), HEAD_DIM)

    def w_cols(half):
        return pl.ds(pl.multiple_of(half * ncol, 128), ncol)

    for j in range(nsp):
        pltpu.make_async_copy(w_ref.at[pl.ds(j * HEAD_DIM, HEAD_DIM), w_cols(c)], wo.at[wo_rows(j, c)], loc.at[0]).start()

    barrier = pltpu.get_barrier_semaphore()
    greet = [dev(xs[i], c, y) for i in (1, 2, 3)]
    greet += [dev(x, ci, ys[i]) for i in (1, 2, 3) for ci in (0, 1)]
    greet.append(dev(x, 1 - c, y))
    for d in greet:
        pl.semaphore_signal(barrier, inc=1, device_id=d, device_id_type=MESH)
    pl.semaphore_wait(barrier, len(greet))

    sends = []

    def go(cp):
        cp.start()
        sends.append(cp)

    partner = dev(x, 1 - c, y)

    def quarter_of(q, g):
        return lax.rem(g + (2, 1, nx - 1, 0)[q], nx)

    def o_rows(q, r):
        return o_ref.at[pl.ds(pl.multiple_of(quarter_of(q, y) * quarter + r * sub, sub), sub)]

    def r_rows(r):
        return pl.ds(pl.multiple_of(r * sub, sub), sub)

    def cell(q, r, xi):
        return og.at[q, r_rows(r), pl.ds(pl.multiple_of(c * kw + xi * width, 128), width)]

    diagonal = x == y

    def attend(q):
        def body(n, carry):
            start = pl.multiple_of(quarter_of(q, y) * quarter + n * bq, bq)
            rows = pl.ds(start, bq)
            ids = jnp.broadcast_to(seg_ref[start // bq], (HEAD_DIM, bq)).T
            top0 = score_rows(qkv_ref[0, rows, :HEAD_DIM], qkv_ref, 0, ids, seg_ref, sc0)
            top1 = score_rows(qkv_ref[1, rows, :HEAD_DIM], qkv_ref, 1, ids, seg_ref, sc1)
            inv0 = exp_rows(sc0, top0)
            o_ref[rows, :HEAD_DIM] = value_rows(sc0, inv0, qkv_ref, 0).astype(BF16)
            inv1 = exp_rows(sc1, top1)
            o_ref[rows, HEAD_DIM:] = value_rows(sc1, inv1, qkv_ref, 1).astype(BF16)
            return carry

        lax.fori_loop(0, quarter // bq, body, 0)

    def stage1(q):
        for i in (1, 2, 3):
            r = ys[i]

            @pl.when(diagonal)
            def _():
                rc(o_rows(q, r), cell(q, r, x), a_s.at[q, i], a_r.at[q, y], dev(x, c, r)).start()

            @pl.when(jnp.logical_not(diagonal))
            def _():
                rc(o_rows(q, r), s1.at[q, y], a_s.at[q, i], a_r.at[q, y], dev(x, c, r)).start()

        @pl.when(diagonal)
        def _():
            cell(q, y, x)[...] = o_rows(q, y)[...]

    def stage2(q):
        @pl.when(jnp.logical_not(diagonal))
        def _():
            rc(o_rows(q, y), cell(q, y, x), b_s.at[q, 0], b_r.at[q, x], dev(y, c, y)).start()

        for i in (1, 2, 3):
            g = ys[i]
            wait(s1.at[q, g], a_r.at[q, g])

            @pl.when(g != x)
            def _():
                rc(s1.at[q, g], cell(q, y, x), b_s.at[q, i], b_r.at[q, x], dev(g, c, y)).start()

    def block(q, r, core):
        return og.at[q, r_rows(r), pl.ds(pl.multiple_of(core * kw, 128), kw)]

    def stage3(q):
        for i in (1, 2, 3):
            wait(cell(q, y, xs[i]), b_r.at[q, xs[i]])

        b = block(q, y, c)
        go(rc(b, b, p_s.at[q, 0], p_r.at[q, 0], partner))
        go(rc(b, b, g_s.at[q, 0], g_r.at[q, 0], dev(x, c, ys[2])))
        go(rc(b, b, g_s.at[q, 1], g_r.at[q, 1], dev(x, c, ys[1])))

    hs = sub // 2

    def pass_on(q):
        d, u = block(q, ys[1], c), block(q, ys[2], c)
        top, bottom = pl.ds(0, hs), pl.ds(hs, hs)
        wait(d, g_r.at[q, 0])
        go(rc(d.at[top], d.at[top], g_s.at[q, 2], g_r.at[q, 2], dev(x, c, ys[2])))
        go(rc(d, d, p_s.at[q, 1], p_r.at[q, 1], partner))
        wait(u, g_r.at[q, 1])
        go(rc(u.at[bottom], u.at[bottom], g_s.at[q, 3], g_r.at[q, 3], dev(x, c, ys[1])))
        go(rc(u, u, p_s.at[q, 2], p_r.at[q, 2], partner))

    def far_block(q):
        b = block(q, ys[3], c)
        wait(b.at[pl.ds(0, hs)], g_r.at[q, 2])
        wait(b.at[pl.ds(hs, hs)], g_r.at[q, 3])
        go(rc(b, b, p_s.at[q, 3], p_r.at[q, 3], partner))

    def from_partner(q, i):
        wait(block(q, ys[i], 1 - c), p_r.at[q, i])

    nt = 256

    def mm(q, start, count):
        rows = pl.ds(start, count)

        def body(n, carry):
            cols = pl.ds(pl.multiple_of(n * nt, nt), nt)
            part[q, rows, cols] = jnp.dot(og[q, rows, :], wo[:, cols], preferred_element_type=F32)
            return carry

        lax.fori_loop(0, ncol // nt, body, 0)

    left, right = dev(xs[1], c, y), dev(xs[2], c, y)
    cl, cr = pl.ds(0, nh), pl.ds(nh, nh)

    def send_far(i):
        r = r_rows(ys[i])
        go(rc(part.at[0, r, cl], far.at[0, r], f_s.at[0, i], f_r.at[0, i], right))
        go(rc(part.at[0, r, cr], far.at[1, r], f_s.at[1, i], f_r.at[1, i], left))

    def send_near_first(q, i):
        r = r_rows(ys[i])
        if q == 1:
            go(rc(part.at[1, r, cr], near.at[0, r, cr], n_s.at[0, 0, i], n_r.at[0, 0, i], right))
        else:
            go(rc(part.at[2, r, cl], near.at[1, r, cl], n_s.at[1, 0, i], n_r.at[1, 0, i], left))

    def send_near_second(i):
        r = r_rows(ys[i])
        wait(far.at[0, r], f_r.at[0, i])
        part[1, r, cl] += far[0, r, :]
        go(rc(part.at[1, r, cl], near.at[0, r, cl], n_s.at[0, 1, i], n_r.at[0, 1, i], right))
        wait(far.at[1, r], f_r.at[1, i])
        part[2, r, cr] += far[1, r, :]
        go(rc(part.at[2, r, cr], near.at[1, r, cr], n_s.at[1, 1, i], n_r.at[1, 1, i], left))

    for j in range(nsp):
        go(rc(w_ref.at[pl.ds(j * HEAD_DIM, HEAD_DIM), w_cols(1 - c)], wo.at[wo_rows(j, c)], w_s.at[j], w_r.at[0], partner))
    attend(0)
    stage1(0)
    attend(1)
    stage1(1)
    stage2(0)
    attend(2)
    stage1(2)
    stage3(0)
    stage2(1)
    half_w = wo.at[pl.ds(0, nsp * HEAD_DIM)]
    wait(half_w, loc.at[0])
    wait(half_w, w_r.at[0])

    def start_of(i):
        return pl.multiple_of(ys[i] * sub, sub)

    from_partner(0, 0)
    mm(0, start_of(0), sub)
    send_far(0)
    attend(3)
    stage1(3)
    pass_on(0)
    stage3(1)
    for i in (1, 2):
        from_partner(0, i)
        mm(0, start_of(i), sub)
        send_far(i)
    stage2(2)
    far_block(0)
    from_partner(0, 3)
    mm(0, start_of(3), sub)
    send_far(3)
    pass_on(1)
    stage3(2)
    stage2(3)
    far_block(1)
    for i in range(4):
        from_partner(1, i)
    mm(1, 0, quarter)
    for i in range(4):
        send_near_first(1, i)
    pass_on(2)
    stage3(3)
    far_block(2)
    for i in range(4):
        from_partner(2, i)
    mm(2, 0, quarter)
    for i in range(4):
        send_near_first(2, i)
    for i in range(3):
        send_near_second(i)
    pass_on(3)
    far_block(3)
    send_near_second(3)
    for i in range(4):
        from_partner(3, i)
    mm(3, 0, quarter)

    ocols = pl.ds(pl.multiple_of((2 * y + c) * ncol, 128), ncol)
    per = sub // out_rows

    def owner(i, u):
        b = ys[i] * per + u
        return b // ntp, lax.rem(b, ntp)

    def ysrc(i, u):
        return ybuf.at[pl.ds(pl.multiple_of((ys[i] * per + u) * out_rows, out_rows), out_rows)]

    def to_owner(i, u):
        ci, yi = owner(i, u)
        mine = jnp.logical_and(ci == c, yi == y)
        remote = rc(ysrc(i, u), y_ref.at[:, ocols], y_s.at[i, u], y_r.at[y, c], dev(x, ci, yi))
        local = pltpu.make_async_copy(ysrc(i, u), y_ref.at[:, ocols], y_s.at[i, u])
        return mine, remote, local

    for i in range(4):
        r = r_rows(ys[i])
        wait(near.at[0, r, cr], n_r.at[0, 0, i])
        wait(near.at[1, r, cl], n_r.at[1, 0, i])
        wait(near.at[0, r, cl], n_r.at[0, 1, i])
        wait(near.at[1, r, cr], n_r.at[1, 1, i])
        ybuf[r, :] = (part[3, r, :] + near[0, r, :] + near[1, r, :]).astype(BF16)
        for u in range(per):
            mine, remote, local = to_owner(i, u)

            @pl.when(mine)
            def _():
                local.start()

            @pl.when(jnp.logical_not(mine))
            def _():
                remote.start()

    for i in range(4):
        for ci in (0, 1):
            if i == 0:
                continue
            wait(y_ref.at[:, pl.ds(pl.multiple_of((2 * ys[i] + ci) * ncol, 128), ncol)], y_r.at[ys[i], ci])
    wait(y_ref.at[:, pl.ds(pl.multiple_of((2 * y + 1 - c) * ncol, 128), ncol)], y_r.at[y, 1 - c])
    for i in range(4):
        for u in range(per):
            mine, remote, local = to_owner(i, u)

            @pl.when(mine)
            def _():
                local.wait()

            @pl.when(jnp.logical_not(mine))
            def _():
                remote.wait_send()
    for cp in sends:
        cp.wait_send()
    for q in range(4):
        for i in (1, 2, 3):
            rc(o_rows(q, ys[i]), s1.at[q, y], a_s.at[q, i], a_r.at[q, y], dev(x, c, ys[i])).wait_send()

            @pl.when(ys[i] != x)
            def _():
                rc(s1.at[q, ys[i]], cell(q, y, x), b_s.at[q, i], b_r.at[q, x], dev(ys[i], c, y)).wait_send()

        @pl.when(jnp.logical_not(diagonal))
        def _():
            rc(o_rows(q, y), cell(q, y, x), b_s.at[q, 0], b_r.at[q, x], dev(y, c, y)).wait_send()


def out_call(nsp, ntp, qkv, seg, w):
    tokens, width = qkv.shape[1], 2 * HEAD_DIM
    krows, wcols = w.shape
    nx = nsp // 2
    quarter, ncol = tokens // nx, wcols // 2
    sub = quarter // ntp
    dma = pltpu.SemaphoreType.DMA
    return pl.pallas_call(
        functools.partial(out_kernel, nsp, ntp),
        name="out",
        out_shape=jax.ShapeDtypeStruct((tokens // (nsp * ntp), ntp * wcols), BF16),
        in_specs=[VM, VM, ANY],
        out_specs=ANY,
        scratch_shapes=[
            pltpu.VMEM((tokens, width), BF16),
            pltpu.VMEM((seg.shape[2], tokens), F32),
            pltpu.VMEM((seg.shape[2], tokens), F32),
            pltpu.VMEM((4, quarter, nsp * width), BF16),
            pltpu.VMEM((4, ntp, sub, width), BF16),
            pltpu.VMEM((2 * krows, ncol), BF16),
            pltpu.VMEM((4, quarter, ncol), F32),
            pltpu.VMEM((2, quarter, ncol // 2), F32),
            pltpu.VMEM((2, quarter, ncol), F32),
            pltpu.VMEM((quarter, ncol), BF16),
            dma((1,)),
            dma((nsp,)), dma((1,)),
            dma((4, 4)), dma((4, 4)),
            dma((4, 4)), dma((4, 4)),
            dma((4, 4)), dma((4, 4)),
            dma((4, 4)), dma((4, 4)),
            dma((2, 4)), dma((2, 4)),
            dma((2, 2, 4)), dma((2, 2, 4)),
            dma((4, 2)), dma((4, 2)),
        ],
        compiler_params=pltpu.CompilerParams(
            collective_id=1, has_side_effects=True, vmem_limit_bytes=60 * 1024 * 1024),
    )(qkv, seg, w)


def solution(mesh):
    nsp, ntp = mesh.shape["sp"], mesh.shape["tp"]

    def device_block(x_block, doc_block, wqkv_block, wout_block):
        rows = x_block.shape[0]
        qkv, _, _, _, segall = qkv_call(nsp, ntp, x_block, doc_block.reshape(1, rows), wqkv_block)
        return out_call(nsp, ntp, qkv, segall, wout_block)

    return jax.shard_map(
        device_block,
        mesh=mesh,
        in_specs=(P(("dp", "sp"), "tp"), P(("dp", "sp")), P("sp", "tp"), P("sp", "tp")),
        out_specs=P(("dp", "sp", "tp"), None),
        check_vma=False,
    )
```

```python
import functools

import jax
import jax.numpy as jnp
from jax import lax
from jax.experimental import pallas as pl
from jax.experimental.pallas import tpu as pltpu
from jax.sharding import PartitionSpec as P

HEAD_DIM = 128
SOFTMAX_SCALE = HEAD_DIM ** -0.5
MESH = pl.DeviceIdType.MESH
HW = 3 * HEAD_DIM
BF16 = jnp.bfloat16
F32 = jnp.float32
ANY = pl.BlockSpec(memory_space=pl.ANY)
VM = pl.BlockSpec(memory_space=pltpu.VMEM)
ROWS_MM = 1024


def _place(nsp, ntp):
    sp, y = lax.axis_index("sp"), lax.axis_index("tp")
    x, c = sp // 2, sp % 2
    nx = nsp // 2
    xs = [x, lax.rem(x + nx - 1, nx), lax.rem(x + 1, nx), lax.rem(x + 2, nx)]
    ys = [y, lax.rem(y + ntp - 1, ntp), lax.rem(y + 1, ntp), lax.rem(y + 2, ntp)]
    return sp, y, c, xs, ys


EXP_SCALE = SOFTMAX_SCALE * 1.4426950408889634


def score_rows(q, k_ref, h, ids, seg_ref, s_ref, chunk=512):
    tokens = k_ref.shape[0]
    width = seg_ref.shape[2]
    top = None
    for n in range(0, tokens, chunk):
        keys = k_ref[n:n + chunk, h * HW + HEAD_DIM:h * HW + 2 * HEAD_DIM]
        s = lax.dot_general(q, keys, (((1,), (1,)), ((), ())), preferred_element_type=F32)
        for g in range(0, chunk, HEAD_DIM):
            at = n + g
            key_ids = seg_ref[at // width, :, at % width:at % width + HEAD_DIM]
            part = jnp.where(ids == key_ids, s[:, g:g + HEAD_DIM], -jnp.inf)
            s_ref[:, at:at + HEAD_DIM] = part
            top = part if top is None else jnp.maximum(top, part)
    return jnp.max(top, axis=-1, keepdims=True)


def exp_rows(s_ref, top):
    total = None
    for g in range(0, s_ref.shape[1], HEAD_DIM):
        e = jnp.exp2((s_ref[:, g:g + HEAD_DIM] - top) * EXP_SCALE)
        s_ref[:, g:g + HEAD_DIM] = e
        total = e if total is None else total + e
    return 1.0 / jnp.sum(total, axis=-1, keepdims=True)


def value_rows(s_ref, inv, v_ref, h, chunk=512):
    o = None
    for n in range(0, s_ref.shape[1], chunk):
        p = (s_ref[:, n:n + chunk] * inv).astype(BF16)
        d = jnp.dot(p, v_ref[n:n + chunk, h * HW + 2 * HEAD_DIM:(h + 1) * HW], preferred_element_type=F32)
        o = d if o is None else o + d
    return o


def out_part(nsp, ntp, qkv_ref, seg_ref, w_ref, y_ref, o_ref, sc0, sc1, og, s1, wo, part, far, near, ybuf,
             loc, w_s, w_r, a_s, a_r, b_s, b_r, g_s, g_r, p_s, p_r, f_s, f_r, n_s, n_r, y_s, y_r):
    sp, y, c, xs, ys = _place(nsp, ntp)
    x = xs[0]
    nx = nsp // 2
    tokens, width = o_ref.shape
    bq = seg_ref.shape[2]
    quarter = tokens // nx
    sub = quarter // ntp
    kw = nx * width
    ncol = wo.shape[1]
    nh = ncol // 2
    out_rows = y_ref.shape[0]

    def dev(xi, ci, yi):
        return {"sp": 2 * xi + ci, "tp": yi}

    def rc(src, dst, ss, rs, to):
        return pltpu.make_async_remote_copy(
            src_ref=src, dst_ref=dst, send_sem=ss, recv_sem=rs, device_id=to, device_id_type=MESH)

    def wait(dst, sem):
        pltpu.make_async_copy(dst, dst, sem).wait()

    nw = nsp // 2

    def wo_rows(j, core):
        return pl.ds(pl.multiple_of((j % 2) * kw + (core * (nx // 2) + j // 2) * width, 128), width)

    def wo_src(j, half):
        return w_ref.at[pl.ds(j * width, width), w_cols(half)]

    def w_cols(half):
        return pl.ds(pl.multiple_of(half * ncol, 128), ncol)

    for j in range(nw):
        pltpu.make_async_copy(wo_src(j, c), wo.at[wo_rows(j, c)], loc.at[0]).start()

    sends = []

    def go(cp):
        cp.start()
        sends.append(cp)

    partner = dev(x, 1 - c, y)

    def quarter_of(q, g, low):
        if q in (0, 3):
            return lax.rem(g + (2 if q == 0 else 0), nx)
        return lax.rem(g + jnp.where(jnp.logical_xor(low, q == 2), 1, nx - 1), nx)

    def o_rows(q, r):
        return o_ref.at[pl.ds(pl.multiple_of(quarter_of(q, y, r < ntp // 2) * quarter + r * sub, sub), sub)]

    def r_rows(r):
        return pl.ds(pl.multiple_of(r * sub, sub), sub)

    def cell(q, r, xi):
        return og.at[q, r_rows(r), pl.ds(pl.multiple_of(c * kw + xi * width, 128), width)]

    diagonal = x == y

    def attend(q):
        def body(n, carry):
            start = pl.multiple_of(quarter_of(q, y, n * bq < quarter // 2) * quarter + n * bq, bq)
            rows = pl.ds(start, bq)
            ids = jnp.broadcast_to(seg_ref[start // bq], (HEAD_DIM, bq)).T
            top0 = score_rows(qkv_ref[rows, :HEAD_DIM], qkv_ref, 0, ids, seg_ref, sc0)
            top1 = score_rows(qkv_ref[rows, HW:HW + HEAD_DIM], qkv_ref, 1, ids, seg_ref, sc1)
            inv0 = exp_rows(sc0, top0)
            o_ref[rows, :HEAD_DIM] = value_rows(sc0, inv0, qkv_ref, 0).astype(BF16)
            inv1 = exp_rows(sc1, top1)
            o_ref[rows, HEAD_DIM:] = value_rows(sc1, inv1, qkv_ref, 1).astype(BF16)
            return carry

        lax.fori_loop(0, quarter // bq, body, 0)

    def stage1(q):
        for i in (1, 2, 3):
            r = ys[i]

            @pl.when(diagonal)
            def _():
                rc(o_rows(q, r), cell(q, r, x), a_s.at[q, i], a_r.at[q, y], dev(x, c, r)).start()

            @pl.when(jnp.logical_not(diagonal))
            def _():
                rc(o_rows(q, r), s1.at[q, y], a_s.at[q, i], a_r.at[q, y], dev(x, c, r)).start()

        @pl.when(diagonal)
        def _():
            cell(q, y, x)[...] = o_rows(q, y)[...]

    def stage2(q):
        @pl.when(jnp.logical_not(diagonal))
        def _():
            rc(o_rows(q, y), cell(q, y, x), b_s.at[q, 0], b_r.at[q, x], dev(y, c, y)).start()

        for i in (1, 2, 3):
            g = ys[i]
            wait(s1.at[q, g], a_r.at[q, g])

            @pl.when(g != x)
            def _():
                rc(s1.at[q, g], cell(q, y, x), b_s.at[q, i], b_r.at[q, x], dev(g, c, y)).start()

    def block(q, r, core):
        return og.at[q, r_rows(r), pl.ds(pl.multiple_of(core * kw, 128), kw)]

    def stage3(q):
        for i in (1, 2, 3):
            wait(cell(q, y, xs[i]), b_r.at[q, xs[i]])

        b = block(q, y, c)
        go(rc(b, b, p_s.at[q, 0], p_r.at[q, 0], partner))
        go(rc(b, b, g_s.at[q, 0], g_r.at[q, 0], dev(x, c, ys[2])))
        go(rc(b, b, g_s.at[q, 1], g_r.at[q, 1], dev(x, c, ys[1])))

    hs = sub // 2

    def pass_on(q):
        d, u = block(q, ys[1], c), block(q, ys[2], c)
        top, bottom = pl.ds(0, hs), pl.ds(hs, hs)
        wait(d, g_r.at[q, 0])
        go(rc(d.at[top], d.at[top], g_s.at[q, 2], g_r.at[q, 2], dev(x, c, ys[2])))
        go(rc(d, d, p_s.at[q, 1], p_r.at[q, 1], partner))
        wait(u, g_r.at[q, 1])
        go(rc(u.at[bottom], u.at[bottom], g_s.at[q, 3], g_r.at[q, 3], dev(x, c, ys[1])))
        go(rc(u, u, p_s.at[q, 2], p_r.at[q, 2], partner))

    def far_block(q):
        b = block(q, ys[3], c)
        wait(b.at[pl.ds(0, hs)], g_r.at[q, 2])
        wait(b.at[pl.ds(hs, hs)], g_r.at[q, 3])
        go(rc(b, b, p_s.at[q, 3], p_r.at[q, 3], partner))

    def from_partner(q, i):
        wait(block(q, ys[i], 1 - c), p_r.at[q, i])

    nt = 256

    def mm(q, start, count):
        rows = pl.ds(start, count)

        def body(n, carry):
            cols = pl.ds(pl.multiple_of(n * nt, nt), nt)
            part[q, rows, cols] = jnp.dot(og[q, rows, :], wo[:, cols], preferred_element_type=F32)
            return carry

        lax.fori_loop(0, ncol // nt, body, 0)

    left, right = dev(xs[1], c, y), dev(xs[2], c, y)
    cl, cr = pl.ds(0, nh), pl.ds(nh, nh)

    def send_far(i):
        r = r_rows(ys[i])
        go(rc(part.at[0, r, cl], far.at[0, r], f_s.at[0, i], f_r.at[0, i], right))
        go(rc(part.at[0, r, cr], far.at[1, r], f_s.at[1, i], f_r.at[1, i], left))

    def towards(q, i):
        d = jnp.where(jnp.logical_xor(ys[i] < ntp // 2, q == 2), 0, 1)
        return d, dev(jnp.where(d == 0, xs[2], xs[1]), c, y)

    def half_cols(d):
        return pl.ds(pl.multiple_of(d * nh, nh), nh)

    def send_near_first(q, i):
        r = r_rows(ys[i])
        d, to = towards(q, i)
        cols = half_cols(1 - d)
        go(rc(part.at[q, r, cols], near.at[d, r, cols], n_s.at[q - 1, 0, i], n_r.at[d, 0, i], to))

    def send_near_second(q, i):
        r = r_rows(ys[i])
        d, to = towards(q, i)
        cols = half_cols(d)
        wait(far.at[d, r], f_r.at[d, i])
        part[q, r, cols] += far[d, r, :]
        go(rc(part.at[q, r, cols], near.at[d, r, cols], n_s.at[q - 1, 1, i], n_r.at[d, 1, i], to))

    for j in range(nw):
        go(rc(wo_src(j, 1 - c), wo.at[wo_rows(j, c)], w_s.at[j], w_r.at[0], partner))

    def finish():
        attend(0)
        stage1(0)
        attend(1)
        stage1(1)
        stage2(0)
        attend(2)
        stage1(2)
        stage3(0)
        stage2(1)
        half_w = wo.at[pl.ds(0, nw * width)]
        wait(half_w, loc.at[0])
        wait(half_w, w_r.at[0])

        def start_of(i):
            return pl.multiple_of(ys[i] * sub, sub)

        def piece(q, i):
            from_partner(q, i)
            mm(q, start_of(i), sub)
            send_far(i) if q == 0 else send_near_first(q, i)

        piece(0, 0)
        attend(3)
        stage1(3)
        stage3(1)
        pass_on(0)
        piece(1, 0)
        stage2(2)
        piece(0, 1)
        piece(0, 2)
        stage3(2)
        far_block(0)
        piece(0, 3)
        stage2(3)
        piece(2, 0)
        pass_on(1)
        piece(1, 1)
        piece(1, 2)
        stage3(3)
        far_block(1)
        piece(1, 3)
        pass_on(2)
        piece(2, 1)
        piece(2, 2)
        far_block(2)
        piece(2, 3)
        for i in range(3):
            send_near_second(1, i)
            send_near_second(2, i)
        pass_on(3)
        far_block(3)
        send_near_second(1, 3)
        send_near_second(2, 3)
        for i in range(4):
            from_partner(3, i)
        mm(3, 0, quarter)

        ocols = pl.ds(pl.multiple_of((2 * y + c) * ncol, 128), ncol)
        per = sub // out_rows

        def owner(i, u):
            b = ys[i] * per + u
            return b // ntp, lax.rem(b, ntp)

        def ysrc(i, u):
            return ybuf.at[pl.ds(pl.multiple_of((ys[i] * per + u) * out_rows, out_rows), out_rows)]

        def to_owner(i, u):
            ci, yi = owner(i, u)
            mine = jnp.logical_and(ci == c, yi == y)
            remote = rc(ysrc(i, u), y_ref.at[:, ocols], y_s.at[i, u], y_r.at[y, c], dev(x, ci, yi))
            local = pltpu.make_async_copy(ysrc(i, u), y_ref.at[:, ocols], y_s.at[i, u])
            return mine, remote, local

        for i in range(4):
            r = r_rows(ys[i])
            wait(near.at[0, r, cr], n_r.at[0, 0, i])
            wait(near.at[1, r, cl], n_r.at[1, 0, i])
            wait(near.at[0, r, cl], n_r.at[0, 1, i])
            wait(near.at[1, r, cr], n_r.at[1, 1, i])
            ybuf[r, :] = (part[3, r, :] + near[0, r, :] + near[1, r, :]).astype(BF16)
            for u in range(per):
                mine, remote, local = to_owner(i, u)

                @pl.when(mine)
                def _():
                    local.start()

                @pl.when(jnp.logical_not(mine))
                def _():
                    remote.start()

        for i in range(4):
            for ci in (0, 1):
                if i == 0:
                    continue
                wait(y_ref.at[:, pl.ds(pl.multiple_of((2 * ys[i] + ci) * ncol, 128), ncol)], y_r.at[ys[i], ci])
        wait(y_ref.at[:, pl.ds(pl.multiple_of((2 * y + 1 - c) * ncol, 128), ncol)], y_r.at[y, 1 - c])
        for i in range(4):
            for u in range(per):
                mine, remote, local = to_owner(i, u)

                @pl.when(mine)
                def _():
                    local.wait()

                @pl.when(jnp.logical_not(mine))
                def _():
                    remote.wait_send()
        for cp in sends:
            cp.wait_send()
        for q in range(4):
            for i in (1, 2, 3):
                rc(o_rows(q, ys[i]), s1.at[q, y], a_s.at[q, i], a_r.at[q, y], dev(x, c, ys[i])).wait_send()

                @pl.when(ys[i] != x)
                def _():
                    rc(s1.at[q, ys[i]], cell(q, y, x), b_s.at[q, i], b_r.at[q, x], dev(ys[i], c, y)).wait_send()

            @pl.when(jnp.logical_not(diagonal))
            def _():
                rc(o_rows(q, y), cell(q, y, x), b_s.at[q, 0], b_r.at[q, x], dev(y, c, y)).wait_send()

    return finish


def block_kernel(nsp, ntp, x_ref, seg_ref, w_ref, wo_ref, y_ref, xall, wall,
                 acc, xbuf, wbuf, xown, segall, qkv, o_ref, sc0, sc1, og, s1, wo, part, far, near, ybuf,
                 loc, xs_s, xs_r, xy_s, xy_r, xp_s, xp_r, xw_s, xw_r, id_s, id_r, *out_sems):
    sp, y, c, xs, ys = _place(nsp, ntp)
    rows, kcols = x_ref.shape
    krows = w_ref.shape[0]
    half, khalf = rows // 2, krows // 2
    tokens = rows * nsp

    def dev(xi, ci, yi):
        return {"sp": 2 * xi + ci, "tp": yi}

    def rc(src, dst, ss, rs, to):
        return pltpu.make_async_remote_copy(
            src_ref=src, dst_ref=dst, send_sem=ss, recv_sem=rs, device_id=to, device_id_type=MESH)

    own_in = pltpu.make_async_copy(x_ref, xown, loc.at[0])
    own_in.start()

    barrier = pltpu.get_barrier_semaphore()
    greet = []
    for i in (1, 2, 3):
        for ci in (0, 1):
            greet.append(dev(xs[i], ci, y))
    greet.append(dev(xs[0], 1 - c, y))
    greet += [dev(xs[0], ci, ys[i]) for i in (1, 2, 3) for ci in (0, 1)]
    for d in greet:
        pl.semaphore_signal(barrier, inc=1, device_id=d, device_id_type=MESH)
    pl.semaphore_wait(barrier, len(greet))

    def go(cp):
        cp.start()

    partner = dev(xs[0], 1 - c, y)
    left, right = (xs[1], c, y), (xs[2], c, y)

    def blk(yi, xi):
        return xall.at[yi, 2 * xi + c]

    go(rc(x_ref, blk(y, xs[0]), xs_s.at[0], xs_r.at[0], dev(*right)))
    go(rc(x_ref, blk(y, xs[0]), xs_s.at[1], xs_r.at[1], dev(*left)))
    go(rc(x_ref, blk(y, xs[0]), xy_s.at[0, 0], xy_r.at[0, 0], dev(xs[0], c, ys[2])))
    go(rc(x_ref, blk(y, xs[0]), xy_s.at[1, 0], xy_r.at[1, 0], dev(xs[0], c, ys[1])))
    go(rc(x_ref, blk(y, xs[0]), xp_s.at[0, 0], xp_r.at[0, 0], partner))
    n = 0
    for i in range(4):
        for ci in (0, 1):
            if i == 0 and ci == 1:
                continue
            cc = (1 - c) if i == 0 else ci
            back = {0: 0, 1: 2, 2: 1, 3: 3}[i]
            go(rc(seg_ref, segall.at[sp], id_s.at[n], id_r.at[back, c], dev(xs[i], cc, y)))
            n += 1

    def wcol(j, num):
        return pl.ds(pl.multiple_of(j * 2 * HW, 128), num * 2 * HW)

    def wrow(p):
        return pl.ds(pl.multiple_of(p * khalf, khalf), khalf)

    twins = (c, 1 - c)

    def w_send(p, i, n):
        go(rc(w_ref.at[wrow(p), wcol(2 * xs[i] + twins[n], 1)], wall.at[sp, wrow(p)],
              xw_s.at[p, i, n], xw_r.at[p, (0, 2, 1, 3)[i], n], dev(xs[i], twins[n], y)))

    for n in (0, 1):
        w_send(0, 3, n)
    for p in (0, 1):
        w_send(p, 0, 1)

    finish = out_part(nsp, ntp, qkv, segall, wo_ref, y_ref, o_ref, sc0, sc1, og, s1, wo, part, far, near, ybuf, *out_sems)

    own_in.wait()
    own_out = pltpu.make_async_copy(xown, blk(y, xs[0]), loc.at[0])
    own_out.start()
    ids = pltpu.make_async_copy(seg_ref, segall.at[sp], loc.at[5])
    ids.start()

    def wait(dst, sem):
        pltpu.make_async_copy(dst, dst, sem).wait()

    def y_send(i):
        go(rc(blk(y, xs[i]), blk(y, xs[i]), xy_s.at[0, i], xy_r.at[0, i], dev(xs[0], c, ys[2])))
        go(rc(blk(y, xs[i]), blk(y, xs[i]), xy_s.at[1, i], xy_r.at[1, i], dev(xs[0], c, ys[1])))

    def to_partner(j, i):
        go(rc(blk(ys[j], xs[i]), blk(ys[j], xs[i]), xp_s.at[j, i], xp_r.at[j, i], partner))

    wait(blk(y, xs[1]), xs_r.at[0])
    go(rc(blk(y, xs[1]).at[pl.ds(0, half)], blk(y, xs[1]).at[pl.ds(0, half)], xs_s.at[2], xs_r.at[2], dev(*right)))
    wait(blk(y, xs[2]), xs_r.at[1])
    go(rc(blk(y, xs[2]).at[pl.ds(half, half)], blk(y, xs[2]).at[pl.ds(half, half)], xs_s.at[3], xs_r.at[3], dev(*left)))
    for n in (0, 1):
        w_send(0, 1, n)
        w_send(0, 2, n)
    w_send(1, 3, 0)
    for n in (0, 1):
        w_send(1, 1, n)
        w_send(1, 2, n)
    w_send(1, 3, 1)
    for i in (1, 2):
        y_send(i)
        to_partner(0, i)

    def y_pass(i):
        wait(blk(ys[1], xs[i]), xy_r.at[0, i])
        if i in (0, 3):
            go(rc(blk(ys[1], xs[i]), blk(ys[1], xs[i]), xy_s.at[2, i], xy_r.at[2, i], dev(xs[0], c, ys[2])))
        to_partner(1, i)
        wait(blk(ys[2], xs[i]), xy_r.at[1, i])
        if i in (1, 2):
            go(rc(blk(ys[2], xs[i]), blk(ys[2], xs[i]), xy_s.at[2, i], xy_r.at[2, i], dev(xs[0], c, ys[1])))
        to_partner(2, i)

    y_pass(0)
    wait(blk(y, xs[3]).at[pl.ds(0, half)], xs_r.at[2])
    wait(blk(y, xs[3]).at[pl.ds(half, half)], xs_r.at[3])
    y_send(3)
    to_partner(0, 3)

    acc[...] = jnp.zeros_like(acc)
    y_pass(1)
    y_pass(2)

    def from_partner(j):
        for i in range(4):
            wait(xall.at[ys[j], 2 * xs[i] + 1 - c], xp_r.at[j, i])

    def w_wait(p, i, n):
        wait(wall.at[2 * xs[i] + twins[n], wrow(p)], xw_r.at[p, i, n])

    def x_load(p, s, slot):
        cols = pl.ds(pl.multiple_of((s % 2) * krows + p * khalf, khalf), khalf)
        for r in range(nsp):
            pltpu.make_async_copy(
                xall.at[s // 2, r, :, cols], xbuf.at[slot, pl.ds(r * rows, rows)], loc.at[1 + slot]).start()

    def w_load(p, s, slot):
        @pl.when(s == sp)
        def _():
            pltpu.make_async_copy(w_ref.at[wrow(p), wcol(sp, 1)], wbuf.at[slot], loc.at[3 + slot]).start()

        @pl.when(s != sp)
        def _():
            pltpu.make_async_copy(wall.at[s, wrow(p)], wbuf.at[slot], loc.at[3 + slot]).start()

    def mm(slot, last):
        def body(rb, carry):
            r = pl.ds(pl.multiple_of(rb * ROWS_MM, ROWS_MM), ROWS_MM)
            total = acc[r, :] + jnp.dot(xbuf[slot, r, :], wbuf[slot], preferred_element_type=F32)
            if last:
                qkv[r, :] = total.astype(BF16)
            else:
                acc[r, :] = total
            return carry

        lax.fori_loop(0, tokens // ROWS_MM, body, 0)

    def x_ready(j):
        def ready():
            if j == 1:
                y_pass(3)
            if j == 3:
                for i in range(4):
                    wait(blk(ys[3], xs[i]), xy_r.at[2, i])
                    to_partner(3, i)
            from_partner(j)
        return ready

    nothing = lambda: None

    def arrived(p, *which):
        def waits():
            for i, n in which:
                w_wait(p, i, n)
        return waits

    steps = [
        (0, 2 * ys[0], nothing, nothing), (0, 2 * ys[0] + 1, nothing, nothing),
        (0, 2 * ys[1], x_ready(1), nothing), (0, 2 * ys[1] + 1, nothing, nothing),
        (0, 2 * ys[2], x_ready(2), nothing), (0, 2 * ys[2] + 1, nothing, nothing),
        (0, 2 * ys[3], x_ready(3), nothing), (0, 2 * ys[3] + 1, nothing, nothing),
        (1, sp, nothing, nothing), (1, 2 * xs[0] + 1 - c, nothing, arrived(1, (0, 1))),
        (1, 2 * xs[3] + c, nothing, arrived(1, (3, 0))),
        (1, 2 * xs[1] + c, nothing, arrived(1, (1, 0))), (1, 2 * xs[2] + c, nothing, arrived(1, (2, 0))),
        (1, 2 * xs[1] + 1 - c, nothing, arrived(1, (1, 1))), (1, 2 * xs[2] + 1 - c, nothing, arrived(1, (2, 1))),
        (1, 2 * xs[3] + 1 - c, nothing, arrived(1, (3, 1))),
    ]
    own_out.wait()
    from_partner(0)
    x_load(0, steps[0][1], 0)
    arrived(0, (0, 1), (3, 0), (3, 1), (1, 0), (2, 0), (1, 1), (2, 1))()

    def pick(k, values):
        out = values[-1]
        for n in range(len(values) - 2, -1, -1):
            out = jnp.where(k == n, values[n], out)
        return out

    def at_step(k, n, act):
        if act is not nothing:
            pl.when(k == n)(act)

    count = len(steps)

    def step(k, carry):
        slot = lax.rem(k, 2)
        p, s = k // (count // 2), pick(k, [st[1] for st in steps])
        after = jnp.minimum(k + 1, count - 1)
        ahead = (after // (count // 2), pick(after, [st[1] for st in steps]), 1 - slot)
        for n, st in enumerate(steps):
            at_step(k, n, st[3])
        w_load(p, s, slot)
        held = [n - 1 for n, st in enumerate(steps) if st[2] is not nothing]
        late = functools.reduce(jnp.logical_or, [k == n for n in held + [count - 1]])

        @pl.when(jnp.logical_not(late))
        def _():
            x_load(*ahead)

        wait(xbuf.at[slot], loc.at[1 + slot])
        wait(wbuf.at[slot], loc.at[3 + slot])

        @pl.when(k < count - 1)
        def _():
            mm(slot, False)

        @pl.when(k == count - 1)
        def _():
            mm(slot, True)

        for n in held:
            @pl.when(k == n)
            def _():
                steps[n + 1][2]()
                x_load(*ahead)

        return carry

    lax.fori_loop(0, count, step, 0)

    for back in (1, 2, 3):
        for ci in (0, 1):
            wait(segall.at[2 * xs[back] + ci], id_r.at[back, ci])
    wait(segall.at[2 * xs[0] + 1 - c], id_r.at[0, 1 - c])
    ids.wait()

    finish()

    for n in range(4):
        wait(x_ref if n < 2 else x_ref.at[pl.ds(0, half)], xs_s.at[n])
        for j in range(3):
            wait(x_ref, xy_s.at[j, n])
        for j in range(4):
            wait(x_ref, xp_s.at[j, n])
    for n in range(nsp - 1):
        wait(seg_ref, id_s.at[n])
    for p in (0, 1):
        wait(wall.at[0, wrow(0)], xw_s.at[p, 0, 1])
        for i in (1, 2, 3):
            for n in (0, 1):
                wait(wall.at[0, wrow(0)], xw_s.at[p, i, n])


def block_call(nsp, ntp, x, seg, w, w_out):
    rows, kcols = x.shape
    krows, ocols = w.shape[0], w_out.shape[1]
    tokens, width = rows * nsp, 2 * HEAD_DIM
    quarter, ncol = tokens // (nsp // 2), ocols // 2
    sub = quarter // ntp
    dma, vmem = pltpu.SemaphoreType.DMA, pltpu.VMEM
    out_shape = (
        jax.ShapeDtypeStruct((tokens // (nsp * ntp), ntp * ocols), BF16),
        jax.ShapeDtypeStruct((ntp, nsp, rows, kcols), BF16),
        jax.ShapeDtypeStruct((nsp, krows, 2 * HW), BF16),
    )
    return pl.pallas_call(
        functools.partial(block_kernel, nsp, ntp),
        name="block",
        out_shape=out_shape,
        in_specs=[ANY] * 4,
        out_specs=(ANY,) * 3,
        scratch_shapes=[
            vmem((tokens, 2 * HW), F32),
            vmem((2, tokens, krows // 2), BF16),
            vmem((2, krows // 2, 2 * HW), BF16),
            vmem((rows, kcols), BF16),
            vmem((nsp, 1, rows), jnp.int32),
            vmem((tokens, 2 * HW), BF16),
            vmem((tokens, width), BF16),
            vmem((rows, tokens), F32), vmem((rows, tokens), F32),
            vmem((4, quarter, nsp * width), BF16),
            vmem((4, ntp, sub, width), BF16),
            vmem((2 * w_out.shape[0], ncol), BF16),
            vmem((4, quarter, ncol), F32),
            vmem((2, quarter, ncol // 2), F32),
            vmem((2, quarter, ncol), F32),
            vmem((quarter, ncol), BF16),
            dma((6,)),
            dma((4,)), dma((4,)),
            dma((3, 4)), dma((3, 4)),
            dma((4, 4)), dma((4, 4)),
            dma((2, 4, 2)), dma((2, 4, 2)),
            dma((7,)), dma((4, 2)),
            dma((1,)),
            dma((nsp // 2,)), dma((1,)),
            dma((4, 4)), dma((4, 4)),
            dma((4, 4)), dma((4, 4)),
            dma((4, 4)), dma((4, 4)),
            dma((4, 4)), dma((4, 4)),
            dma((2, 4)), dma((2, 4)),
            dma((2, 2, 4)), dma((2, 2, 4)),
            dma((4, 2)), dma((4, 2)),
        ],
        compiler_params=pltpu.CompilerParams(
            collective_id=0, has_side_effects=True, vmem_limit_bytes=62 * 1024 * 1024),
    )(x, seg, w, w_out)[0]


def solution(mesh):
    nsp, ntp = mesh.shape["sp"], mesh.shape["tp"]

    def device_block(x_block, doc_block, wqkv_block, wout_block):
        return block_call(nsp, ntp, x_block, doc_block.reshape(1, -1), wqkv_block, wout_block)

    return jax.shard_map(
        device_block,
        mesh=mesh,
        in_specs=(P(("dp", "sp"), "tp"), P(("dp", "sp")), P("sp", "tp"), P("sp", "tp")),
        out_specs=P(("dp", "sp", "tp"), None),
        check_vma=False,
    )
```

```python
import functools

import jax
import jax.numpy as jnp
from jax import lax
from jax.experimental import pallas as pl
from jax.experimental.pallas import tpu as pltpu
from jax.sharding import PartitionSpec as P

HEAD_DIM = 128
SOFTMAX_SCALE = HEAD_DIM ** -0.5
MESH = pl.DeviceIdType.MESH
HW = 3 * HEAD_DIM
BF16 = jnp.bfloat16
F32 = jnp.float32
ANY = pl.BlockSpec(memory_space=pl.ANY)
VM = pl.BlockSpec(memory_space=pltpu.VMEM)
ROWS_MM = 1024


def _place(nsp, ntp):
    sp, y = lax.axis_index("sp"), lax.axis_index("tp")
    x, c = sp // 2, sp % 2
    nx = nsp // 2
    xs = [x, lax.rem(x + nx - 1, nx), lax.rem(x + 1, nx), lax.rem(x + 2, nx)]
    ys = [y, lax.rem(y + ntp - 1, ntp), lax.rem(y + 1, ntp), lax.rem(y + 2, ntp)]
    return sp, y, c, xs, ys


EXP_SCALE = SOFTMAX_SCALE * 1.4426950408889634


def score_rows(q, k_ref, h, ids, seg_ref, s_ref, chunk=512):
    tokens = k_ref.shape[0]
    width = seg_ref.shape[2]
    top = None
    for n in range(0, tokens, chunk):
        keys = k_ref[n:n + chunk, h * HW + HEAD_DIM:h * HW + 2 * HEAD_DIM]
        s = lax.dot_general(q, keys, (((1,), (1,)), ((), ())), preferred_element_type=F32)
        for g in range(0, chunk, HEAD_DIM):
            at = n + g
            key_ids = seg_ref[at // width, :, at % width:at % width + HEAD_DIM]
            part = jnp.where(ids == key_ids, s[:, g:g + HEAD_DIM], -jnp.inf)
            s_ref[:, at:at + HEAD_DIM] = part
            top = part if top is None else jnp.maximum(top, part)
    return jnp.max(top, axis=-1, keepdims=True)


def exp_rows(s_ref, top):
    total = None
    for g in range(0, s_ref.shape[1], HEAD_DIM):
        e = jnp.exp2((s_ref[:, g:g + HEAD_DIM] - top) * EXP_SCALE)
        s_ref[:, g:g + HEAD_DIM] = e
        total = e if total is None else total + e
    return 1.0 / jnp.sum(total, axis=-1, keepdims=True)


def value_rows(s_ref, inv, v_ref, h, chunk=512):
    o = None
    for n in range(0, s_ref.shape[1], chunk):
        p = (s_ref[:, n:n + chunk] * inv).astype(BF16)
        d = jnp.dot(p, v_ref[n:n + chunk, h * HW + 2 * HEAD_DIM:(h + 1) * HW], preferred_element_type=F32)
        o = d if o is None else o + d
    return o


def out_part(nsp, ntp, qkv_ref, seg_ref, w_ref, y_ref, o_ref, sc0, sc1, og, s1, wo, part, far, near, ybuf,
             loc, w_s, w_r, a_s, a_r, b_s, b_r, g_s, g_r, p_s, p_r, f_s, f_r, n_s, n_r, y_s, y_r):
    sp, y, c, xs, ys = _place(nsp, ntp)
    x = xs[0]
    nx = nsp // 2
    tokens, width = o_ref.shape
    bq = seg_ref.shape[2]
    quarter = tokens // nx
    sub = quarter // ntp
    kw = nx * width
    ncol = wo.shape[1]
    nh = ncol // 2
    out_rows = y_ref.shape[0]

    def dev(xi, ci, yi):
        return {"sp": 2 * xi + ci, "tp": yi}

    def rc(src, dst, ss, rs, to):
        return pltpu.make_async_remote_copy(
            src_ref=src, dst_ref=dst, send_sem=ss, recv_sem=rs, device_id=to, device_id_type=MESH)

    def wait(dst, sem):
        pltpu.make_async_copy(dst, dst, sem).wait()

    nw = nsp // 2

    def wo_rows(j, core):
        return pl.ds(pl.multiple_of((j % 2) * kw + (core * (nx // 2) + j // 2) * width, 128), width)

    def wo_src(j, half):
        return w_ref.at[pl.ds(j * width, width), w_cols(half)]

    def w_cols(half):
        return pl.ds(pl.multiple_of(half * ncol, 128), ncol)

    for j in range(nw):
        pltpu.make_async_copy(wo_src(j, c), wo.at[wo_rows(j, c)], loc.at[0]).start()

    sends = []

    def go(cp):
        cp.start()
        sends.append(cp)

    partner = dev(x, 1 - c, y)

    def quarter_of(q, g, low):
        if q in (0, 3):
            return lax.rem(g + (2 if q == 0 else 0), nx)
        return lax.rem(g + jnp.where(jnp.logical_xor(low, q == 2), 1, nx - 1), nx)

    def o_rows(q, r):
        return o_ref.at[pl.ds(pl.multiple_of(quarter_of(q, y, r < ntp // 2) * quarter + r * sub, sub), sub)]

    def r_rows(r):
        return pl.ds(pl.multiple_of(r * sub, sub), sub)

    def cell(q, r, xi):
        return og.at[q, r_rows(r), pl.ds(pl.multiple_of(c * kw + xi * width, 128), width)]

    diagonal = x == y

    def attend(q, first=0, last=None):
        def body(n, carry):
            start = pl.multiple_of(quarter_of(q, y, n * bq < quarter // 2) * quarter + n * bq, bq)
            rows = pl.ds(start, bq)
            ids = jnp.broadcast_to(seg_ref[start // bq], (HEAD_DIM, bq)).T
            top0 = score_rows(qkv_ref[rows, :HEAD_DIM], qkv_ref, 0, ids, seg_ref, sc0)
            top1 = score_rows(qkv_ref[rows, HW:HW + HEAD_DIM], qkv_ref, 1, ids, seg_ref, sc1)
            inv0 = exp_rows(sc0, top0)
            o_ref[rows, :HEAD_DIM] = value_rows(sc0, inv0, qkv_ref, 0).astype(BF16)
            inv1 = exp_rows(sc1, top1)
            o_ref[rows, HEAD_DIM:] = value_rows(sc1, inv1, qkv_ref, 1).astype(BF16)
            return carry

        lax.fori_loop(first, quarter // bq if last is None else last, body, 0)

    def stage1(q):
        for i in (1, 2, 3):
            r = ys[i]

            @pl.when(diagonal)
            def _():
                rc(o_rows(q, r), cell(q, r, x), a_s.at[q, i], a_r.at[q, y], dev(x, c, r)).start()

            @pl.when(jnp.logical_not(diagonal))
            def _():
                rc(o_rows(q, r), s1.at[q, y], a_s.at[q, i], a_r.at[q, y], dev(x, c, r)).start()

        @pl.when(diagonal)
        def _():
            cell(q, y, x)[...] = o_rows(q, y)[...]

    def stage2(q):
        @pl.when(jnp.logical_not(diagonal))
        def _():
            rc(o_rows(q, y), cell(q, y, x), b_s.at[q, 0], b_r.at[q, x], dev(y, c, y)).start()

        for i in (1, 2, 3):
            g = ys[i]
            wait(s1.at[q, g], a_r.at[q, g])

            @pl.when(g != x)
            def _():
                rc(s1.at[q, g], cell(q, y, x), b_s.at[q, i], b_r.at[q, x], dev(g, c, y)).start()

    def block(q, r, core):
        return og.at[q, r_rows(r), pl.ds(pl.multiple_of(core * kw, 128), kw)]

    def stage3(q):
        for i in (1, 2, 3):
            wait(cell(q, y, xs[i]), b_r.at[q, xs[i]])

        b = block(q, y, c)
        go(rc(b, b, p_s.at[q, 0], p_r.at[q, 0], partner))
        go(rc(b, b, g_s.at[q, 0], g_r.at[q, 0], dev(x, c, ys[2])))
        go(rc(b, b, g_s.at[q, 1], g_r.at[q, 1], dev(x, c, ys[1])))

    hs = sub // 2

    def pass_on(q):
        d, u = block(q, ys[1], c), block(q, ys[2], c)
        top, bottom = pl.ds(0, hs), pl.ds(hs, hs)
        wait(d, g_r.at[q, 0])
        go(rc(d.at[top], d.at[top], g_s.at[q, 2], g_r.at[q, 2], dev(x, c, ys[2])))
        go(rc(d, d, p_s.at[q, 1], p_r.at[q, 1], partner))
        wait(u, g_r.at[q, 1])
        go(rc(u.at[bottom], u.at[bottom], g_s.at[q, 3], g_r.at[q, 3], dev(x, c, ys[1])))
        go(rc(u, u, p_s.at[q, 2], p_r.at[q, 2], partner))

    def far_block(q):
        b = block(q, ys[3], c)
        wait(b.at[pl.ds(0, hs)], g_r.at[q, 2])
        wait(b.at[pl.ds(hs, hs)], g_r.at[q, 3])
        go(rc(b, b, p_s.at[q, 3], p_r.at[q, 3], partner))

    def from_partner(q, i):
        wait(block(q, ys[i], 1 - c), p_r.at[q, i])

    nt = 256

    def mm(q, start, count):
        rows = pl.ds(start, count)

        def body(n, carry):
            cols = pl.ds(pl.multiple_of(n * nt, nt), nt)
            part[q, rows, cols] = jnp.dot(og[q, rows, :], wo[:, cols], preferred_element_type=F32)
            return carry

        lax.fori_loop(0, ncol // nt, body, 0)

    left, right = dev(xs[1], c, y), dev(xs[2], c, y)
    cl, cr = pl.ds(0, nh), pl.ds(nh, nh)

    def send_far(i):
        r = r_rows(ys[i])
        go(rc(part.at[0, r, cl], far.at[0, r], f_s.at[0, i], f_r.at[0, i], right))
        go(rc(part.at[0, r, cr], far.at[1, r], f_s.at[1, i], f_r.at[1, i], left))

    def towards(q, i):
        d = jnp.where(jnp.logical_xor(ys[i] < ntp // 2, q == 2), 0, 1)
        return d, dev(jnp.where(d == 0, xs[2], xs[1]), c, y)

    def half_cols(d):
        return pl.ds(pl.multiple_of(d * nh, nh), nh)

    def send_near_first(q, i):
        r = r_rows(ys[i])
        d, to = towards(q, i)
        cols = half_cols(1 - d)
        go(rc(part.at[q, r, cols], near.at[d, r, cols], n_s.at[q - 1, 0, i], n_r.at[d, 0, i], to))

    def send_near_second(q, i):
        r = r_rows(ys[i])
        d, to = towards(q, i)
        cols = half_cols(d)
        wait(far.at[d, r], f_r.at[d, i])
        part[q, r, cols] += far[d, r, :]
        go(rc(part.at[q, r, cols], near.at[d, r, cols], n_s.at[q - 1, 1, i], n_r.at[d, 1, i], to))

    for j in range(nw):
        go(rc(wo_src(j, 1 - c), wo.at[wo_rows(j, c)], w_s.at[j], w_r.at[0], partner))

    def finish():
        attend(0)
        stage1(0)
        attend(1)
        stage1(1)
        stage2(0)
        attend(2)
        stage1(2)
        stage3(0)
        stage2(1)
        half_w = wo.at[pl.ds(0, nw * width)]
        wait(half_w, loc.at[0])
        wait(half_w, w_r.at[0])

        def start_of(i):
            return pl.multiple_of(ys[i] * sub, sub)

        def piece(q, i):
            from_partner(q, i)
            mm(q, start_of(i), sub)
            send_far(i) if q == 0 else send_near_first(q, i)

        piece(0, 0)
        attend(3)
        stage1(3)
        stage3(1)
        pass_on(0)
        stage2(2)
        piece(1, 0)
        piece(0, 1)
        piece(0, 2)
        far_block(0)
        stage3(2)
        stage2(3)
        pass_on(1)
        piece(0, 3)
        piece(1, 1)
        piece(1, 2)
        stage3(3)
        far_block(1)
        pass_on(2)
        piece(2, 0)
        piece(1, 3)
        send_near_second(1, 0)
        send_near_second(1, 1)
        send_near_second(1, 2)
        far_block(2)
        pass_on(3)
        piece(2, 1)
        piece(2, 2)
        send_near_second(1, 3)
        far_block(3)
        piece(2, 3)
        send_near_second(2, 0)
        send_near_second(2, 1)
        send_near_second(2, 2)
        send_near_second(2, 3)
        for i in range(4):
            from_partner(3, i)
        mm(3, 0, quarter)

        ocols = pl.ds(pl.multiple_of((2 * y + c) * ncol, 128), ncol)
        per = sub // out_rows

        def owner(i, u):
            b = ys[i] * per + u
            return b // ntp, lax.rem(b, ntp)

        def ysrc(i, u):
            return ybuf.at[pl.ds(pl.multiple_of((ys[i] * per + u) * out_rows, out_rows), out_rows)]

        def to_owner(i, u):
            ci, yi = owner(i, u)
            mine = jnp.logical_and(ci == c, yi == y)
            remote = rc(ysrc(i, u), y_ref.at[:, ocols], y_s.at[i, u], y_r.at[y, c], dev(x, ci, yi))
            local = pltpu.make_async_copy(ysrc(i, u), y_ref.at[:, ocols], y_s.at[i, u])
            return mine, remote, local

        for i in range(4):
            r = r_rows(ys[i])
            wait(near.at[0, r, cr], n_r.at[0, 0, i])
            wait(near.at[1, r, cl], n_r.at[1, 0, i])
            wait(near.at[0, r, cl], n_r.at[0, 1, i])
            wait(near.at[1, r, cr], n_r.at[1, 1, i])
            ybuf[r, :] = (part[3, r, :] + near[0, r, :] + near[1, r, :]).astype(BF16)
            for u in range(per):
                mine, remote, local = to_owner(i, u)

                @pl.when(mine)
                def _():
                    local.start()

                @pl.when(jnp.logical_not(mine))
                def _():
                    remote.start()

        for i in range(4):
            for ci in (0, 1):
                if i == 0:
                    continue
                wait(y_ref.at[:, pl.ds(pl.multiple_of((2 * ys[i] + ci) * ncol, 128), ncol)], y_r.at[ys[i], ci])
        wait(y_ref.at[:, pl.ds(pl.multiple_of((2 * y + 1 - c) * ncol, 128), ncol)], y_r.at[y, 1 - c])
        for i in range(4):
            for u in range(per):
                mine, remote, local = to_owner(i, u)

                @pl.when(mine)
                def _():
                    local.wait()

                @pl.when(jnp.logical_not(mine))
                def _():
                    remote.wait_send()
        for cp in sends:
            cp.wait_send()
        for q in range(4):
            for i in (1, 2, 3):
                rc(o_rows(q, ys[i]), s1.at[q, y], a_s.at[q, i], a_r.at[q, y], dev(x, c, ys[i])).wait_send()

                @pl.when(ys[i] != x)
                def _():
                    rc(s1.at[q, ys[i]], cell(q, y, x), b_s.at[q, i], b_r.at[q, x], dev(ys[i], c, y)).wait_send()

            @pl.when(jnp.logical_not(diagonal))
            def _():
                rc(o_rows(q, y), cell(q, y, x), b_s.at[q, 0], b_r.at[q, x], dev(y, c, y)).wait_send()

    return finish


def block_kernel(nsp, ntp, x_ref, seg_ref, w_ref, wo_ref, y_ref, xall, wall, wst,
                 acc, xbuf, wbuf, xown, segall, qkv, o_ref, sc0, sc1, og, s1, wo, part, far, near, ybuf,
                 loc, xs_s, xs_r, xy_s, xy_r, xp_s, xp_r, xw_s, xw_r, xf_s, xf_r, id_s, id_r, *out_sems):
    sp, y, c, xs, ys = _place(nsp, ntp)
    rows, kcols = x_ref.shape
    krows = w_ref.shape[0]
    half, khalf = rows // 2, krows // 2
    tokens = rows * nsp

    def dev(xi, ci, yi):
        return {"sp": 2 * xi + ci, "tp": yi}

    def rc(src, dst, ss, rs, to):
        return pltpu.make_async_remote_copy(
            src_ref=src, dst_ref=dst, send_sem=ss, recv_sem=rs, device_id=to, device_id_type=MESH)

    own_in = pltpu.make_async_copy(x_ref, xown, loc.at[0])
    own_in.start()

    barrier = pltpu.get_barrier_semaphore()
    greet = []
    for i in (1, 2, 3):
        for ci in (0, 1):
            greet.append(dev(xs[i], ci, y))
    greet.append(dev(xs[0], 1 - c, y))
    greet += [dev(xs[0], ci, ys[i]) for i in (1, 2, 3) for ci in (0, 1)]
    for d in greet:
        pl.semaphore_signal(barrier, inc=1, device_id=d, device_id_type=MESH)
    pl.semaphore_wait(barrier, len(greet))

    def wait(dst, sem):
        pltpu.make_async_copy(dst, dst, sem).wait()

    def go(cp):
        cp.start()

    partner = dev(xs[0], 1 - c, y)
    left, right = (xs[1], c, y), (xs[2], c, y)

    def blk(yi, xi):
        return xall.at[yi, 2 * xi + c]

    go(rc(x_ref, blk(y, xs[0]), xs_s.at[0], xs_r.at[0], dev(*right)))
    go(rc(x_ref, blk(y, xs[0]), xs_s.at[1], xs_r.at[1], dev(*left)))
    go(rc(x_ref, blk(y, xs[0]), xy_s.at[0, 0], xy_r.at[0, 0], dev(xs[0], c, ys[2])))
    go(rc(x_ref, blk(y, xs[0]), xy_s.at[1, 0], xy_r.at[1, 0], dev(xs[0], c, ys[1])))
    go(rc(x_ref, blk(y, xs[0]), xp_s.at[0, 0], xp_r.at[0, 0], partner))
    n = 0
    for i in range(4):
        for ci in (0, 1):
            if i == 0 and ci == 1:
                continue
            cc = (1 - c) if i == 0 else ci
            back = {0: 0, 1: 2, 2: 1, 3: 3}[i]
            go(rc(seg_ref, segall.at[sp], id_s.at[n], id_r.at[back, c], dev(xs[i], cc, y)))
            n += 1

    def wcol(j, num):
        return pl.ds(pl.multiple_of(j * 2 * HW, 128), num * 2 * HW)

    def wrow(p):
        return pl.ds(pl.multiple_of(p * khalf, khalf), khalf)

    twins = (c, 1 - c)

    def w_send(p, i, n):
        go(rc(w_ref.at[wrow(p), wcol(2 * xs[i] + twins[n], 1)], wall.at[sp, wrow(p)],
              xw_s.at[p, i, n], xw_r.at[p, (0, 2, 1)[i], n], dev(xs[i], twins[n], y)))

    kfar = khalf // 2

    def far_rows(p, d):
        return pl.ds(p * khalf + d * kfar, kfar)

    def w_far(p):
        for d, to in enumerate((right, left)):
            go(rc(w_ref.at[far_rows(p, d), wcol(2 * xs[3], 2)], wst.at[d, p], xf_s.at[p, d], xf_r.at[p, d], dev(*to)))

    def w_pass(p):
        for d in (0, 1):
            wait(wst.at[d, p], xf_r.at[p, d])
        for n in (0, 1):
            cols = pl.ds(pl.multiple_of(twins[n] * 2 * HW, 128), 2 * HW)
            for d, i in enumerate((2, 1)):
                go(rc(wst.at[d, p, :, cols], wall.at[2 * xs[3 - i] + c, far_rows(p, d)],
                      xw_s.at[p, 3 + d, n], xw_r.at[p, 3 + d, n], dev(xs[i], twins[n], y)))

    def w_near(p):
        for n in (0, 1):
            w_send(p, 1, n)
            w_send(p, 2, n)

    w_far(0)
    for p in (0, 1):
        w_send(p, 0, 1)

    finish = out_part(nsp, ntp, qkv, segall, wo_ref, y_ref, o_ref, sc0, sc1, og, s1, wo, part, far, near, ybuf, *out_sems)

    own_in.wait()
    own_out = pltpu.make_async_copy(xown, blk(y, xs[0]), loc.at[0])
    own_out.start()
    ids = pltpu.make_async_copy(seg_ref, segall.at[sp], loc.at[5])
    ids.start()

    def y_send(i):
        go(rc(blk(y, xs[i]), blk(y, xs[i]), xy_s.at[0, i], xy_r.at[0, i], dev(xs[0], c, ys[2])))
        go(rc(blk(y, xs[i]), blk(y, xs[i]), xy_s.at[1, i], xy_r.at[1, i], dev(xs[0], c, ys[1])))

    def to_partner(j, i):
        go(rc(blk(ys[j], xs[i]), blk(ys[j], xs[i]), xp_s.at[j, i], xp_r.at[j, i], partner))

    wait(blk(y, xs[1]), xs_r.at[0])
    go(rc(blk(y, xs[1]).at[pl.ds(0, half)], blk(y, xs[1]).at[pl.ds(0, half)], xs_s.at[2], xs_r.at[2], dev(*right)))
    wait(blk(y, xs[2]), xs_r.at[1])
    go(rc(blk(y, xs[2]).at[pl.ds(half, half)], blk(y, xs[2]).at[pl.ds(half, half)], xs_s.at[3], xs_r.at[3], dev(*left)))
    w_near(0)
    for i in (1, 2):
        y_send(i)
        to_partner(0, i)

    def y_pass(i):
        wait(blk(ys[1], xs[i]), xy_r.at[0, i])
        if i in (0, 3):
            go(rc(blk(ys[1], xs[i]), blk(ys[1], xs[i]), xy_s.at[2, i], xy_r.at[2, i], dev(xs[0], c, ys[2])))
        to_partner(1, i)
        wait(blk(ys[2], xs[i]), xy_r.at[1, i])
        if i in (1, 2):
            go(rc(blk(ys[2], xs[i]), blk(ys[2], xs[i]), xy_s.at[2, i], xy_r.at[2, i], dev(xs[0], c, ys[1])))
        to_partner(2, i)

    y_pass(0)
    w_pass(0)
    w_far(1)
    w_near(1)
    wait(blk(y, xs[3]).at[pl.ds(0, half)], xs_r.at[2])
    wait(blk(y, xs[3]).at[pl.ds(half, half)], xs_r.at[3])
    y_send(3)
    to_partner(0, 3)

    acc[...] = jnp.zeros_like(acc)
    y_pass(1)
    y_pass(2)

    def from_partner(j):
        for i in range(4):
            wait(xall.at[ys[j], 2 * xs[i] + 1 - c], xp_r.at[j, i])

    def w_wait(p, i, n):
        if i < 3:
            wait(wall.at[2 * xs[i] + twins[n], wrow(p)], xw_r.at[p, i, n])
        else:
            for d in (0, 1):
                wait(wall.at[2 * xs[3] + twins[n], far_rows(p, d)], xw_r.at[p, 3 + d, n])

    def x_load(p, s, slot):
        cols = pl.ds(pl.multiple_of((s % 2) * krows + p * khalf, khalf), khalf)
        for r in range(nsp):
            pltpu.make_async_copy(
                xall.at[s // 2, r, :, cols], xbuf.at[slot, pl.ds(r * rows, rows)], loc.at[1 + slot]).start()

    def w_load(p, s, slot):
        @pl.when(s == sp)
        def _():
            pltpu.make_async_copy(w_ref.at[wrow(p), wcol(sp, 1)], wbuf.at[slot], loc.at[3 + slot]).start()

        @pl.when(s != sp)
        def _():
            pltpu.make_async_copy(wall.at[s, wrow(p)], wbuf.at[slot], loc.at[3 + slot]).start()

    def mm(slot, last):
        def body(rb, carry):
            r = pl.ds(pl.multiple_of(rb * ROWS_MM, ROWS_MM), ROWS_MM)
            total = acc[r, :] + jnp.dot(xbuf[slot, r, :], wbuf[slot], preferred_element_type=F32)
            if last:
                qkv[r, :] = total.astype(BF16)
            else:
                acc[r, :] = total
            return carry

        lax.fori_loop(0, tokens // ROWS_MM, body, 0)

    def x_ready(j):
        def ready():
            if j == 1:
                y_pass(3)
            if j == 3:
                for i in range(4):
                    wait(blk(ys[3], xs[i]), xy_r.at[2, i])
                    to_partner(3, i)
            from_partner(j)
        return ready

    nothing = lambda: None

    def arrived(p, *which):
        def waits():
            for i, n in which:
                w_wait(p, i, n)
        return waits

    steps = [
        (0, 2 * ys[0], nothing, nothing), (0, 2 * ys[0] + 1, nothing, nothing),
        (0, 2 * ys[1], x_ready(1), nothing), (0, 2 * ys[1] + 1, nothing, nothing),
        (0, 2 * ys[2], x_ready(2), nothing), (0, 2 * ys[2] + 1, nothing, nothing),
        (0, 2 * ys[3], x_ready(3), lambda: w_pass(1)), (0, 2 * ys[3] + 1, nothing, nothing),
        (1, sp, nothing, nothing), (1, 2 * xs[0] + 1 - c, nothing, arrived(1, (0, 1))),
        (1, 2 * xs[1] + c, nothing, arrived(1, (1, 0))), (1, 2 * xs[2] + c, nothing, arrived(1, (2, 0))),
        (1, 2 * xs[1] + 1 - c, nothing, arrived(1, (1, 1))), (1, 2 * xs[2] + 1 - c, nothing, arrived(1, (2, 1))),
        (1, 2 * xs[3] + c, nothing, arrived(1, (3, 0))),
        (1, 2 * xs[3] + 1 - c, nothing, arrived(1, (3, 1))),
    ]
    own_out.wait()
    from_partner(0)
    x_load(0, steps[0][1], 0)
    arrived(0, (0, 1), (3, 0), (3, 1), (1, 0), (2, 0), (1, 1), (2, 1))()

    def pick(k, values):
        out = values[-1]
        for n in range(len(values) - 2, -1, -1):
            out = jnp.where(k == n, values[n], out)
        return out

    def at_step(k, n, act):
        if act is not nothing:
            pl.when(k == n)(act)

    count = len(steps)

    def step(k, carry):
        slot = lax.rem(k, 2)
        p, s = k // (count // 2), pick(k, [st[1] for st in steps])
        after = jnp.minimum(k + 1, count - 1)
        ahead = (after // (count // 2), pick(after, [st[1] for st in steps]), 1 - slot)
        for n, st in enumerate(steps):
            at_step(k, n, st[3])
        w_load(p, s, slot)
        held = [n - 1 for n, st in enumerate(steps) if st[2] is not nothing]
        late = functools.reduce(jnp.logical_or, [k == n for n in held + [count - 1]])

        @pl.when(jnp.logical_not(late))
        def _():
            x_load(*ahead)

        wait(xbuf.at[slot], loc.at[1 + slot])
        wait(wbuf.at[slot], loc.at[3 + slot])

        @pl.when(k < count - 1)
        def _():
            mm(slot, False)

        @pl.when(k == count - 1)
        def _():
            mm(slot, True)

        for n in held:
            @pl.when(k == n)
            def _():
                steps[n + 1][2]()
                x_load(*ahead)

        return carry

    lax.fori_loop(0, count, step, 0)

    for back in (1, 2, 3):
        for ci in (0, 1):
            wait(segall.at[2 * xs[back] + ci], id_r.at[back, ci])
    wait(segall.at[2 * xs[0] + 1 - c], id_r.at[0, 1 - c])
    ids.wait()

    finish()

    for n in range(4):
        wait(x_ref if n < 2 else x_ref.at[pl.ds(0, half)], xs_s.at[n])
        for j in range(3):
            wait(x_ref, xy_s.at[j, n])
        for j in range(4):
            wait(x_ref, xp_s.at[j, n])
    for n in range(nsp - 1):
        wait(seg_ref, id_s.at[n])
    for p in (0, 1):
        wait(wall.at[0, wrow(0)], xw_s.at[p, 0, 1])
        for n in (0, 1):
            for i in (1, 2):
                wait(wall.at[0, wrow(0)], xw_s.at[p, i, n])
            for d in (0, 1):
                wait(wall.at[0, far_rows(0, 0)], xw_s.at[p, 3 + d, n])
                if n == 0:
                    wait(wst.at[0, 0], xf_s.at[p, d])


def block_call(nsp, ntp, x, seg, w, w_out):
    rows, kcols = x.shape
    krows, ocols = w.shape[0], w_out.shape[1]
    tokens, width = rows * nsp, 2 * HEAD_DIM
    quarter, ncol = tokens // (nsp // 2), ocols // 2
    sub = quarter // ntp
    dma, vmem = pltpu.SemaphoreType.DMA, pltpu.VMEM
    out_shape = (
        jax.ShapeDtypeStruct((tokens // (nsp * ntp), ntp * ocols), BF16),
        jax.ShapeDtypeStruct((ntp, nsp, rows, kcols), BF16),
        jax.ShapeDtypeStruct((nsp, krows, 2 * HW), BF16),
        jax.ShapeDtypeStruct((2, 2, krows // 4, 4 * HW), BF16),
    )
    return pl.pallas_call(
        functools.partial(block_kernel, nsp, ntp),
        name="block",
        out_shape=out_shape,
        in_specs=[ANY] * 4,
        out_specs=(ANY,) * 4,
        scratch_shapes=[
            vmem((tokens, 2 * HW), F32),
            vmem((2, tokens, krows // 2), BF16),
            vmem((2, krows // 2, 2 * HW), BF16),
            vmem((rows, kcols), BF16),
            vmem((nsp, 1, rows), jnp.int32),
            vmem((tokens, 2 * HW), BF16),
            vmem((tokens, width), BF16),
            vmem((rows, tokens), F32), vmem((rows, tokens), F32),
            vmem((4, quarter, nsp * width), BF16),
            vmem((4, ntp, sub, width), BF16),
            vmem((2 * w_out.shape[0], ncol), BF16),
            vmem((4, quarter, ncol), F32),
            vmem((2, quarter, ncol // 2), F32),
            vmem((2, quarter, ncol), F32),
            vmem((quarter, ncol), BF16),
            dma((6,)),
            dma((4,)), dma((4,)),
            dma((3, 4)), dma((3, 4)),
            dma((4, 4)), dma((4, 4)),
            dma((2, 5, 2)), dma((2, 5, 2)),
            dma((2, 2)), dma((2, 2)),
            dma((7,)), dma((4, 2)),
            dma((1,)),
            dma((nsp // 2,)), dma((1,)),
            dma((4, 4)), dma((4, 4)),
            dma((4, 4)), dma((4, 4)),
            dma((4, 4)), dma((4, 4)),
            dma((4, 4)), dma((4, 4)),
            dma((2, 4)), dma((2, 4)),
            dma((2, 2, 4)), dma((2, 2, 4)),
            dma((4, 2)), dma((4, 2)),
        ],
        compiler_params=pltpu.CompilerParams(
            collective_id=0, has_side_effects=True, vmem_limit_bytes=62 * 1024 * 1024),
    )(x, seg, w, w_out)[0]


def solution(mesh):
    nsp, ntp = mesh.shape["sp"], mesh.shape["tp"]

    def device_block(x_block, doc_block, wqkv_block, wout_block):
        return block_call(nsp, ntp, x_block, doc_block.reshape(1, -1), wqkv_block, wout_block)

    return jax.shard_map(
        device_block,
        mesh=mesh,
        in_specs=(P(("dp", "sp"), "tp"), P(("dp", "sp")), P("sp", "tp"), P("sp", "tp")),
        out_specs=P(("dp", "sp", "tp"), None),
        check_vma=False,
    )
```

```python
import functools

import jax
import jax.numpy as jnp
from jax import lax
from jax.experimental import pallas as pl
from jax.experimental.pallas import tpu as pltpu
from jax.sharding import PartitionSpec as P

HEAD_DIM = 128
SOFTMAX_SCALE = HEAD_DIM ** -0.5
MESH = pl.DeviceIdType.MESH
HW = 3 * HEAD_DIM
BF16 = jnp.bfloat16
F32 = jnp.float32
ANY = pl.BlockSpec(memory_space=pl.ANY)
VM = pl.BlockSpec(memory_space=pltpu.VMEM)
ROWS_MM = 1024


def _place(nsp, ntp):
    sp, y = lax.axis_index("sp"), lax.axis_index("tp")
    x, c = sp // 2, sp % 2
    nx = nsp // 2
    xs = [x, lax.rem(x + nx - 1, nx), lax.rem(x + 1, nx), lax.rem(x + 2, nx)]
    ys = [y, lax.rem(y + ntp - 1, ntp), lax.rem(y + 1, ntp), lax.rem(y + 2, ntp)]
    return sp, y, c, xs, ys


EXP_SCALE = SOFTMAX_SCALE * 1.4426950408889634


def score_rows(q, k_ref, h, ids, seg_ref, s_ref, chunk=512):
    tokens = k_ref.shape[0]
    width = seg_ref.shape[2]
    top = None
    for n in range(0, tokens, chunk):
        keys = k_ref[n:n + chunk, h * HW + HEAD_DIM:h * HW + 2 * HEAD_DIM]
        s = lax.dot_general(q, keys, (((1,), (1,)), ((), ())), preferred_element_type=F32)
        for g in range(0, chunk, HEAD_DIM):
            at = n + g
            key_ids = seg_ref[at // width, :, at % width:at % width + HEAD_DIM]
            part = jnp.where(ids == key_ids, s[:, g:g + HEAD_DIM], -jnp.inf)
            s_ref[:, at:at + HEAD_DIM] = part
            top = part if top is None else jnp.maximum(top, part)
    return jnp.max(top, axis=-1, keepdims=True)


def exp_rows(s_ref, top):
    total = None
    for g in range(0, s_ref.shape[1], HEAD_DIM):
        e = jnp.exp2((s_ref[:, g:g + HEAD_DIM] - top) * EXP_SCALE)
        s_ref[:, g:g + HEAD_DIM] = e
        total = e if total is None else total + e
    return 1.0 / jnp.sum(total, axis=-1, keepdims=True)


def value_rows(s_ref, inv, v_ref, h, chunk=512):
    o = None
    for n in range(0, s_ref.shape[1], chunk):
        p = (s_ref[:, n:n + chunk] * inv).astype(BF16)
        d = jnp.dot(p, v_ref[n:n + chunk, h * HW + 2 * HEAD_DIM:(h + 1) * HW], preferred_element_type=F32)
        o = d if o is None else o + d
    return o


def out_part(nsp, ntp, qkv_ref, seg_ref, w_ref, y_ref, o_ref, sc0, sc1, og, s1, wo, part, far, near, ybuf,
             loc, w_s, w_r, a_s, a_r, b_s, b_r, g_s, g_r, p_s, p_r, f_s, f_r, n_s, n_r, y_s, y_r):
    sp, y, c, xs, ys = _place(nsp, ntp)
    x = xs[0]
    nx = nsp // 2
    tokens, width = o_ref.shape
    bq = seg_ref.shape[2]
    quarter = tokens // nx
    sub = quarter // ntp
    kw = nx * width
    ncol = wo.shape[1]
    nh = ncol // 2
    out_rows = y_ref.shape[0]

    def dev(xi, ci, yi):
        return {"sp": 2 * xi + ci, "tp": yi}

    def rc(src, dst, ss, rs, to):
        return pltpu.make_async_remote_copy(
            src_ref=src, dst_ref=dst, send_sem=ss, recv_sem=rs, device_id=to, device_id_type=MESH)

    def wait(dst, sem):
        pltpu.make_async_copy(dst, dst, sem).wait()

    nw = nsp // 2

    def wo_rows(j, core):
        return pl.ds(pl.multiple_of((j % 2) * kw + (core * (nx // 2) + j // 2) * width, 128), width)

    def wo_src(j, half):
        return w_ref.at[pl.ds(j * width, width), w_cols(half)]

    def w_cols(half):
        return pl.ds(pl.multiple_of(half * ncol, 128), ncol)

    for j in range(nw):
        pltpu.make_async_copy(wo_src(j, c), wo.at[wo_rows(j, c)], loc.at[0]).start()

    sends = []

    def go(cp):
        cp.start()
        sends.append(cp)

    partner = dev(x, 1 - c, y)

    def quarter_of(q, g, low):
        if q in (0, 3):
            return lax.rem(g + (2 if q == 0 else 0), nx)
        return lax.rem(g + jnp.where(jnp.logical_xor(low, q == 2), 1, nx - 1), nx)

    def o_rows(q, r):
        return o_ref.at[pl.ds(pl.multiple_of(quarter_of(q, y, r < ntp // 2) * quarter + r * sub, sub), sub)]

    def r_rows(r):
        return pl.ds(pl.multiple_of(r * sub, sub), sub)

    def cell(q, r, xi):
        return og.at[q, r_rows(r), pl.ds(pl.multiple_of(c * kw + xi * width, 128), width)]

    diagonal = x == y

    def attend(q, first=0, last=None):
        def body(n, carry):
            start = pl.multiple_of(quarter_of(q, y, n * bq < quarter // 2) * quarter + n * bq, bq)
            rows = pl.ds(start, bq)
            ids = jnp.broadcast_to(seg_ref[start // bq], (HEAD_DIM, bq)).T
            top0 = score_rows(qkv_ref[rows, :HEAD_DIM], qkv_ref, 0, ids, seg_ref, sc0)
            top1 = score_rows(qkv_ref[rows, HW:HW + HEAD_DIM], qkv_ref, 1, ids, seg_ref, sc1)
            inv0 = exp_rows(sc0, top0)
            o_ref[rows, :HEAD_DIM] = value_rows(sc0, inv0, qkv_ref, 0).astype(BF16)
            inv1 = exp_rows(sc1, top1)
            o_ref[rows, HEAD_DIM:] = value_rows(sc1, inv1, qkv_ref, 1).astype(BF16)
            return carry

        lax.fori_loop(first, quarter // bq if last is None else last, body, 0)

    def stage1(q):
        for i in (1, 2, 3):
            r = ys[i]

            @pl.when(diagonal)
            def _():
                rc(o_rows(q, r), cell(q, r, x), a_s.at[q, i], a_r.at[q, y], dev(x, c, r)).start()

            @pl.when(jnp.logical_not(diagonal))
            def _():
                rc(o_rows(q, r), s1.at[q, y], a_s.at[q, i], a_r.at[q, y], dev(x, c, r)).start()

        @pl.when(diagonal)
        def _():
            cell(q, y, x)[...] = o_rows(q, y)[...]

    def stage2(q):
        @pl.when(jnp.logical_not(diagonal))
        def _():
            rc(o_rows(q, y), cell(q, y, x), b_s.at[q, 0], b_r.at[q, x], dev(y, c, y)).start()

        for i in (1, 2, 3):
            g = ys[i]
            wait(s1.at[q, g], a_r.at[q, g])

            @pl.when(g != x)
            def _():
                rc(s1.at[q, g], cell(q, y, x), b_s.at[q, i], b_r.at[q, x], dev(g, c, y)).start()

    def block(q, r, core):
        return og.at[q, r_rows(r), pl.ds(pl.multiple_of(core * kw, 128), kw)]

    def stage3(q):
        for i in (1, 2, 3):
            wait(cell(q, y, xs[i]), b_r.at[q, xs[i]])

        b = block(q, y, c)
        go(rc(b, b, p_s.at[q, 0], p_r.at[q, 0], partner))
        go(rc(b, b, g_s.at[q, 0], g_r.at[q, 0], dev(x, c, ys[2])))
        go(rc(b, b, g_s.at[q, 1], g_r.at[q, 1], dev(x, c, ys[1])))

    hs = sub // 2

    def pass_on(q):
        d, u = block(q, ys[1], c), block(q, ys[2], c)
        top, bottom = pl.ds(0, hs), pl.ds(hs, hs)
        wait(d, g_r.at[q, 0])
        go(rc(d.at[top], d.at[top], g_s.at[q, 2], g_r.at[q, 2], dev(x, c, ys[2])))
        go(rc(d, d, p_s.at[q, 1], p_r.at[q, 1], partner))
        wait(u, g_r.at[q, 1])
        go(rc(u.at[bottom], u.at[bottom], g_s.at[q, 3], g_r.at[q, 3], dev(x, c, ys[1])))
        go(rc(u, u, p_s.at[q, 2], p_r.at[q, 2], partner))

    def far_block(q):
        b = block(q, ys[3], c)
        wait(b.at[pl.ds(0, hs)], g_r.at[q, 2])
        wait(b.at[pl.ds(hs, hs)], g_r.at[q, 3])
        go(rc(b, b, p_s.at[q, 3], p_r.at[q, 3], partner))

    def from_partner(q, i):
        wait(block(q, ys[i], 1 - c), p_r.at[q, i])

    nt = 256

    def mm(q, start, count):
        rows = pl.ds(start, count)

        def body(n, carry):
            cols = pl.ds(pl.multiple_of(n * nt, nt), nt)
            part[q, rows, cols] = jnp.dot(og[q, rows, :], wo[:, cols], preferred_element_type=F32)
            return carry

        lax.fori_loop(0, ncol // nt, body, 0)

    left, right = dev(xs[1], c, y), dev(xs[2], c, y)
    cl, cr = pl.ds(0, nh), pl.ds(nh, nh)

    def send_far(i):
        r = r_rows(ys[i])
        go(rc(part.at[0, r, cl], far.at[0, r], f_s.at[0, i], f_r.at[0, i], right))
        go(rc(part.at[0, r, cr], far.at[1, r], f_s.at[1, i], f_r.at[1, i], left))

    def towards(q, i):
        d = jnp.where(jnp.logical_xor(ys[i] < ntp // 2, q == 2), 0, 1)
        return d, dev(jnp.where(d == 0, xs[2], xs[1]), c, y)

    def half_cols(d):
        return pl.ds(pl.multiple_of(d * nh, nh), nh)

    def send_near_first(q, i):
        r = r_rows(ys[i])
        d, to = towards(q, i)
        cols = half_cols(1 - d)
        go(rc(part.at[q, r, cols], near.at[d, r, cols], n_s.at[q - 1, 0, i], n_r.at[d, 0, i], to))

    def send_near_second(q, i):
        r = r_rows(ys[i])
        d, to = towards(q, i)
        cols = half_cols(d)
        wait(far.at[d, r], f_r.at[d, i])
        part[q, r, cols] += far[d, r, :]
        go(rc(part.at[q, r, cols], near.at[d, r, cols], n_s.at[q - 1, 1, i], n_r.at[d, 1, i], to))

    for j in range(nw):
        go(rc(wo_src(j, 1 - c), wo.at[wo_rows(j, c)], w_s.at[j], w_r.at[0], partner))

    def finish():
        attend(0)
        stage1(0)
        attend(1)
        stage1(1)
        stage2(0)
        attend(2)
        stage1(2)
        stage3(0)
        stage2(1)
        half_w = wo.at[pl.ds(0, nw * width)]
        wait(half_w, loc.at[0])
        wait(half_w, w_r.at[0])

        def start_of(i):
            return pl.multiple_of(ys[i] * sub, sub)

        def piece(q, i):
            from_partner(q, i)
            mm(q, start_of(i), sub)
            send_far(i) if q == 0 else send_near_first(q, i)

        piece(0, 0)
        attend(3)
        stage1(3)
        stage3(1)
        pass_on(0)
        stage2(2)
        piece(1, 0)
        piece(0, 1)
        piece(0, 2)
        far_block(0)
        stage3(2)
        stage2(3)
        pass_on(1)
        piece(0, 3)
        piece(1, 1)
        piece(1, 2)
        stage3(3)
        far_block(1)
        pass_on(2)
        piece(2, 0)
        piece(1, 3)
        send_near_second(1, 0)
        send_near_second(1, 1)
        send_near_second(1, 2)
        far_block(2)
        pass_on(3)
        piece(2, 1)
        piece(2, 2)
        send_near_second(1, 3)
        far_block(3)
        piece(2, 3)
        send_near_second(2, 0)
        send_near_second(2, 1)
        send_near_second(2, 2)
        send_near_second(2, 3)
        for i in range(4):
            from_partner(3, i)
        mm(3, 0, quarter)

        ocols = pl.ds(pl.multiple_of((2 * y + c) * ncol, 128), ncol)
        per = sub // out_rows

        def owner(i, u):
            b = ys[i] * per + u
            return b // ntp, lax.rem(b, ntp)

        def ysrc(i, u):
            return ybuf.at[pl.ds(pl.multiple_of((ys[i] * per + u) * out_rows, out_rows), out_rows)]

        def to_owner(i, u):
            ci, yi = owner(i, u)
            mine = jnp.logical_and(ci == c, yi == y)
            remote = rc(ysrc(i, u), y_ref.at[:, ocols], y_s.at[i, u], y_r.at[y, c], dev(x, ci, yi))
            local = pltpu.make_async_copy(ysrc(i, u), y_ref.at[:, ocols], y_s.at[i, u])
            return mine, remote, local

        for i in range(4):
            r = r_rows(ys[i])
            wait(near.at[0, r, cr], n_r.at[0, 0, i])
            wait(near.at[1, r, cl], n_r.at[1, 0, i])
            wait(near.at[0, r, cl], n_r.at[0, 1, i])
            wait(near.at[1, r, cr], n_r.at[1, 1, i])
            ybuf[r, :] = (part[3, r, :] + near[0, r, :] + near[1, r, :]).astype(BF16)
            for u in range(per):
                mine, remote, local = to_owner(i, u)

                @pl.when(mine)
                def _():
                    local.start()

                @pl.when(jnp.logical_not(mine))
                def _():
                    remote.start()

        for i in range(4):
            for ci in (0, 1):
                if i == 0:
                    continue
                wait(y_ref.at[:, pl.ds(pl.multiple_of((2 * ys[i] + ci) * ncol, 128), ncol)], y_r.at[ys[i], ci])
        wait(y_ref.at[:, pl.ds(pl.multiple_of((2 * y + 1 - c) * ncol, 128), ncol)], y_r.at[y, 1 - c])
        for i in range(4):
            for u in range(per):
                mine, remote, local = to_owner(i, u)

                @pl.when(mine)
                def _():
                    local.wait()

                @pl.when(jnp.logical_not(mine))
                def _():
                    remote.wait_send()
        for cp in sends:
            cp.wait_send()
        for q in range(4):
            for i in (1, 2, 3):
                rc(o_rows(q, ys[i]), s1.at[q, y], a_s.at[q, i], a_r.at[q, y], dev(x, c, ys[i])).wait_send()

                @pl.when(ys[i] != x)
                def _():
                    rc(s1.at[q, ys[i]], cell(q, y, x), b_s.at[q, i], b_r.at[q, x], dev(ys[i], c, y)).wait_send()

            @pl.when(jnp.logical_not(diagonal))
            def _():
                rc(o_rows(q, y), cell(q, y, x), b_s.at[q, 0], b_r.at[q, x], dev(y, c, y)).wait_send()

    return finish


def block_kernel(nsp, ntp, x_ref, seg_ref, w_ref, wo_ref, y_ref, xall, wall, wst,
                 acc, xbuf, wbuf, wlast, xown, segall, qkv, o_ref, sc0, sc1, og, s1, wo, part, far, near, ybuf,
                 loc, xs_s, xs_r, xy_s, xy_r, xp_s, xp_r, xw_s, xw_r, xf_s, xf_r, id_s, id_r, *out_sems):
    sp, y, c, xs, ys = _place(nsp, ntp)
    rows, kcols = x_ref.shape
    krows = w_ref.shape[0]
    half, khalf = rows // 2, krows // 2
    tokens = rows * nsp

    def dev(xi, ci, yi):
        return {"sp": 2 * xi + ci, "tp": yi}

    def rc(src, dst, ss, rs, to):
        return pltpu.make_async_remote_copy(
            src_ref=src, dst_ref=dst, send_sem=ss, recv_sem=rs, device_id=to, device_id_type=MESH)

    own_in = pltpu.make_async_copy(x_ref, xown, loc.at[0])
    own_in.start()

    barrier = pltpu.get_barrier_semaphore()
    greet = []
    for i in (1, 2, 3):
        for ci in (0, 1):
            greet.append(dev(xs[i], ci, y))
    greet.append(dev(xs[0], 1 - c, y))
    greet += [dev(xs[0], ci, ys[i]) for i in (1, 2, 3) for ci in (0, 1)]
    for d in greet:
        pl.semaphore_signal(barrier, inc=1, device_id=d, device_id_type=MESH)
    pl.semaphore_wait(barrier, len(greet))

    def wait(dst, sem):
        pltpu.make_async_copy(dst, dst, sem).wait()

    def go(cp):
        cp.start()

    partner = dev(xs[0], 1 - c, y)
    left, right = (xs[1], c, y), (xs[2], c, y)

    def blk(yi, xi):
        return xall.at[yi, 2 * xi + c]

    go(rc(x_ref, blk(y, xs[0]), xs_s.at[0], xs_r.at[0], dev(*right)))
    go(rc(x_ref, blk(y, xs[0]), xs_s.at[1], xs_r.at[1], dev(*left)))
    go(rc(x_ref, blk(y, xs[0]), xy_s.at[0, 0], xy_r.at[0, 0], dev(xs[0], c, ys[2])))
    go(rc(x_ref, blk(y, xs[0]), xy_s.at[1, 0], xy_r.at[1, 0], dev(xs[0], c, ys[1])))
    go(rc(x_ref, blk(y, xs[0]), xp_s.at[0, 0], xp_r.at[0, 0], partner))
    n = 0
    for i in range(4):
        for ci in (0, 1):
            if i == 0 and ci == 1:
                continue
            cc = (1 - c) if i == 0 else ci
            back = {0: 0, 1: 2, 2: 1, 3: 3}[i]
            go(rc(seg_ref, segall.at[sp], id_s.at[n], id_r.at[back, c], dev(xs[i], cc, y)))
            n += 1

    def wcol(j, num):
        return pl.ds(pl.multiple_of(j * 2 * HW, 128), num * 2 * HW)

    def wrow(p):
        return pl.ds(pl.multiple_of(p * khalf, khalf), khalf)

    twins = (c, 1 - c)

    def w_send(p, i, n):
        go(rc(w_ref.at[wrow(p), wcol(2 * xs[i] + twins[n], 1)], wall.at[sp, wrow(p)],
              xw_s.at[p, i, n], xw_r.at[p, (0, 2, 1)[i], n], dev(xs[i], twins[n], y)))

    kfar = khalf // 2

    def far_rows(p, d):
        return pl.ds(p * khalf + d * kfar, kfar)

    def w_far(p):
        for d, to in enumerate((right, left)):
            go(rc(w_ref.at[far_rows(p, d), wcol(2 * xs[3], 2)], wst.at[d, p], xf_s.at[p, d], xf_r.at[p, d], dev(*to)))

    def w_pass(p):
        for d in (0, 1):
            wait(wst.at[d, p], xf_r.at[p, d])
        for n in (0, 1):
            cols = pl.ds(pl.multiple_of(twins[n] * 2 * HW, 128), 2 * HW)
            for d, i in enumerate((2, 1)):
                dst = wlast.at[pl.ds(d * kfar, kfar)] if (p, n) == (1, 1) else wall.at[2 * xs[3 - i] + c, far_rows(p, d)]
                go(rc(wst.at[d, p, :, cols], dst,
                      xw_s.at[p, 3 + d, n], xw_r.at[p, 3 + d, n], dev(xs[i], twins[n], y)))

    def w_near(p):
        for n in (0, 1):
            w_send(p, 1, n)
            w_send(p, 2, n)

    w_far(0)
    for p in (0, 1):
        w_send(p, 0, 1)

    finish = out_part(nsp, ntp, qkv, segall, wo_ref, y_ref, o_ref, sc0, sc1, og, s1, wo, part, far, near, ybuf, *out_sems)

    own_in.wait()
    own_out = pltpu.make_async_copy(xown, blk(y, xs[0]), loc.at[0])
    own_out.start()
    ids = pltpu.make_async_copy(seg_ref, segall.at[sp], loc.at[5])
    ids.start()

    def y_send(i):
        go(rc(blk(y, xs[i]), blk(y, xs[i]), xy_s.at[0, i], xy_r.at[0, i], dev(xs[0], c, ys[2])))
        go(rc(blk(y, xs[i]), blk(y, xs[i]), xy_s.at[1, i], xy_r.at[1, i], dev(xs[0], c, ys[1])))

    def to_partner(j, i):
        go(rc(blk(ys[j], xs[i]), blk(ys[j], xs[i]), xp_s.at[j, i], xp_r.at[j, i], partner))

    wait(blk(y, xs[1]), xs_r.at[0])
    go(rc(blk(y, xs[1]).at[pl.ds(0, half)], blk(y, xs[1]).at[pl.ds(0, half)], xs_s.at[2], xs_r.at[2], dev(*right)))
    wait(blk(y, xs[2]), xs_r.at[1])
    go(rc(blk(y, xs[2]).at[pl.ds(half, half)], blk(y, xs[2]).at[pl.ds(half, half)], xs_s.at[3], xs_r.at[3], dev(*left)))
    w_near(0)
    for i in (1, 2):
        y_send(i)
        to_partner(0, i)

    def y_pass(i):
        wait(blk(ys[1], xs[i]), xy_r.at[0, i])
        if i in (0, 3):
            go(rc(blk(ys[1], xs[i]), blk(ys[1], xs[i]), xy_s.at[2, i], xy_r.at[2, i], dev(xs[0], c, ys[2])))
        to_partner(1, i)
        wait(blk(ys[2], xs[i]), xy_r.at[1, i])
        if i in (1, 2):
            go(rc(blk(ys[2], xs[i]), blk(ys[2], xs[i]), xy_s.at[2, i], xy_r.at[2, i], dev(xs[0], c, ys[1])))
        to_partner(2, i)

    y_pass(0)
    w_pass(0)
    w_far(1)
    w_near(1)
    wait(blk(y, xs[3]).at[pl.ds(0, half)], xs_r.at[2])
    wait(blk(y, xs[3]).at[pl.ds(half, half)], xs_r.at[3])
    y_send(3)
    to_partner(0, 3)

    acc[...] = jnp.zeros_like(acc)
    y_pass(1)
    y_pass(2)

    def from_partner(j):
        for i in range(4):
            wait(xall.at[ys[j], 2 * xs[i] + 1 - c], xp_r.at[j, i])

    def w_wait(p, i, n):
        if i < 3:
            wait(wall.at[2 * xs[i] + twins[n], wrow(p)], xw_r.at[p, i, n])
        else:
            for d in (0, 1):
                got = wlast.at[pl.ds(d * kfar, kfar)] if (p, n) == (1, 1) else wall.at[2 * xs[3] + twins[n], far_rows(p, d)]
                wait(got, xw_r.at[p, 3 + d, n])

    def x_load(p, s, slot):
        cols = pl.ds(pl.multiple_of((s % 2) * krows + p * khalf, khalf), khalf)
        for r in range(nsp):
            pltpu.make_async_copy(
                xall.at[s // 2, r, :, cols], xbuf.at[slot, pl.ds(r * rows, rows)], loc.at[1 + slot]).start()

    def w_load(p, s, slot):
        @pl.when(s == sp)
        def _():
            pltpu.make_async_copy(w_ref.at[wrow(p), wcol(sp, 1)], wbuf.at[slot], loc.at[3 + slot]).start()

        @pl.when(s != sp)
        def _():
            pltpu.make_async_copy(wall.at[s, wrow(p)], wbuf.at[slot], loc.at[3 + slot]).start()

    def mm(slot, last):
        def body(rb, carry):
            r = pl.ds(pl.multiple_of(rb * ROWS_MM, ROWS_MM), ROWS_MM)
            total = acc[r, :] + jnp.dot(xbuf[slot, r, :], wlast[...] if last else wbuf[slot], preferred_element_type=F32)
            if last:
                qkv[r, :] = total.astype(BF16)
            else:
                acc[r, :] = total
            return carry

        lax.fori_loop(0, tokens // ROWS_MM, body, 0)

    def x_ready(j):
        def ready():
            if j == 1:
                y_pass(3)
            if j == 3:
                for i in range(4):
                    wait(blk(ys[3], xs[i]), xy_r.at[2, i])
                    to_partner(3, i)
            from_partner(j)
        return ready

    nothing = lambda: None

    def arrived(p, *which):
        def waits():
            for i, n in which:
                w_wait(p, i, n)
        return waits

    steps = [
        (0, 2 * ys[0], nothing, nothing), (0, 2 * ys[0] + 1, nothing, nothing),
        (0, 2 * ys[1], x_ready(1), nothing), (0, 2 * ys[1] + 1, nothing, nothing),
        (0, 2 * ys[2], x_ready(2), nothing), (0, 2 * ys[2] + 1, nothing, nothing),
        (0, 2 * ys[3], x_ready(3), lambda: w_pass(1)), (0, 2 * ys[3] + 1, nothing, nothing),
        (1, sp, nothing, nothing), (1, 2 * xs[0] + 1 - c, nothing, arrived(1, (0, 1))),
        (1, 2 * xs[1] + c, nothing, arrived(1, (1, 0))), (1, 2 * xs[2] + c, nothing, arrived(1, (2, 0))),
        (1, 2 * xs[1] + 1 - c, nothing, arrived(1, (1, 1))), (1, 2 * xs[2] + 1 - c, nothing, arrived(1, (2, 1))),
        (1, 2 * xs[3] + c, nothing, arrived(1, (3, 0))),
        (1, 2 * xs[3] + 1 - c, nothing, arrived(1, (3, 1))),
    ]
    own_out.wait()
    from_partner(0)
    x_load(0, steps[0][1], 0)
    arrived(0, (0, 1), (3, 0), (3, 1), (1, 0), (2, 0), (1, 1), (2, 1))()

    def pick(k, values):
        out = values[-1]
        for n in range(len(values) - 2, -1, -1):
            out = jnp.where(k == n, values[n], out)
        return out

    def at_step(k, n, act):
        if act is not nothing:
            pl.when(k == n)(act)

    count = len(steps)

    def step(k, carry):
        slot = lax.rem(k, 2)
        p, s = k // (count // 2), pick(k, [st[1] for st in steps])
        after = jnp.minimum(k + 1, count - 1)
        ahead = (after // (count // 2), pick(after, [st[1] for st in steps]), 1 - slot)
        for n, st in enumerate(steps):
            at_step(k, n, st[3])

        @pl.when(k < count - 1)
        def _():
            w_load(p, s, slot)

        held = [n - 1 for n, st in enumerate(steps) if st[2] is not nothing]
        late = functools.reduce(jnp.logical_or, [k == n for n in held + [count - 1]])

        @pl.when(jnp.logical_not(late))
        def _():
            x_load(*ahead)

        wait(xbuf.at[slot], loc.at[1 + slot])

        @pl.when(k < count - 1)
        def _():
            wait(wbuf.at[slot], loc.at[3 + slot])
            mm(slot, False)

        @pl.when(k == count - 1)
        def _():
            mm(slot, True)

        for n in held:
            @pl.when(k == n)
            def _():
                steps[n + 1][2]()
                x_load(*ahead)

        return carry

    lax.fori_loop(0, count, step, 0)

    for back in (1, 2, 3):
        for ci in (0, 1):
            wait(segall.at[2 * xs[back] + ci], id_r.at[back, ci])
    wait(segall.at[2 * xs[0] + 1 - c], id_r.at[0, 1 - c])
    ids.wait()

    finish()

    for n in range(4):
        wait(x_ref if n < 2 else x_ref.at[pl.ds(0, half)], xs_s.at[n])
        for j in range(3):
            wait(x_ref, xy_s.at[j, n])
        for j in range(4):
            wait(x_ref, xp_s.at[j, n])
    for n in range(nsp - 1):
        wait(seg_ref, id_s.at[n])
    for p in (0, 1):
        wait(wall.at[0, wrow(0)], xw_s.at[p, 0, 1])
        for n in (0, 1):
            for i in (1, 2):
                wait(wall.at[0, wrow(0)], xw_s.at[p, i, n])
            for d in (0, 1):
                wait(wall.at[0, far_rows(0, 0)], xw_s.at[p, 3 + d, n])
                if n == 0:
                    wait(wst.at[0, 0], xf_s.at[p, d])


def block_call(nsp, ntp, x, seg, w, w_out):
    rows, kcols = x.shape
    krows, ocols = w.shape[0], w_out.shape[1]
    tokens, width = rows * nsp, 2 * HEAD_DIM
    quarter, ncol = tokens // (nsp // 2), ocols // 2
    sub = quarter // ntp
    dma, vmem = pltpu.SemaphoreType.DMA, pltpu.VMEM
    out_shape = (
        jax.ShapeDtypeStruct((tokens // (nsp * ntp), ntp * ocols), BF16),
        jax.ShapeDtypeStruct((ntp, nsp, rows, kcols), BF16),
        jax.ShapeDtypeStruct((nsp, krows, 2 * HW), BF16),
        jax.ShapeDtypeStruct((2, 2, krows // 4, 4 * HW), BF16),
    )
    return pl.pallas_call(
        functools.partial(block_kernel, nsp, ntp),
        name="block",
        out_shape=out_shape,
        in_specs=[ANY] * 4,
        out_specs=(ANY,) * 4,
        scratch_shapes=[
            vmem((tokens, 2 * HW), F32),
            vmem((2, tokens, krows // 2), BF16),
            vmem((2, krows // 2, 2 * HW), BF16),
            vmem((krows // 2, 2 * HW), BF16),
            vmem((rows, kcols), BF16),
            vmem((nsp, 1, rows), jnp.int32),
            vmem((tokens, 2 * HW), BF16),
            vmem((tokens, width), BF16),
            vmem((rows, tokens), F32), vmem((rows, tokens), F32),
            vmem((4, quarter, nsp * width), BF16),
            vmem((4, ntp, sub, width), BF16),
            vmem((2 * w_out.shape[0], ncol), BF16),
            vmem((4, quarter, ncol), F32),
            vmem((2, quarter, ncol // 2), F32),
            vmem((2, quarter, ncol), F32),
            vmem((quarter, ncol), BF16),
            dma((6,)),
            dma((4,)), dma((4,)),
            dma((3, 4)), dma((3, 4)),
            dma((4, 4)), dma((4, 4)),
            dma((2, 5, 2)), dma((2, 5, 2)),
            dma((2, 2)), dma((2, 2)),
            dma((7,)), dma((4, 2)),
            dma((1,)),
            dma((nsp // 2,)), dma((1,)),
            dma((4, 4)), dma((4, 4)),
            dma((4, 4)), dma((4, 4)),
            dma((4, 4)), dma((4, 4)),
            dma((4, 4)), dma((4, 4)),
            dma((2, 4)), dma((2, 4)),
            dma((2, 2, 4)), dma((2, 2, 4)),
            dma((4, 2)), dma((4, 2)),
        ],
        compiler_params=pltpu.CompilerParams(
            collective_id=0, has_side_effects=True, vmem_limit_bytes=62 * 1024 * 1024),
    )(x, seg, w, w_out)[0]


def copy_kernel(src_ref, dst_ref):
    dst_ref[...] = src_ref[...]


def place(y, parts):
    rows, cols = y.shape
    block = pl.BlockSpec((rows, cols // parts), lambda i: (0, i))
    return pl.pallas_call(
        copy_kernel, name="place", grid=(parts,), in_specs=[block], out_specs=block,
        out_shape=jax.ShapeDtypeStruct(y.shape, y.dtype))(y)


def solution(mesh):
    nsp, ntp = mesh.shape["sp"], mesh.shape["tp"]

    def device_block(x_block, doc_block, wqkv_block, wout_block):
        y_block = block_call(nsp, ntp, x_block, doc_block.reshape(1, -1), wqkv_block, wout_block)
        return place(y_block, ntp)

    return jax.shard_map(
        device_block,
        mesh=mesh,
        in_specs=(P(("dp", "sp"), "tp"), P(("dp", "sp")), P("sp", "tp"), P("sp", "tp")),
        out_specs=P(("dp", "sp", "tp"), None),
        check_vma=False,
    )
```
